32 devices in a mesh: seq: 8 (over z, core), tp: 2 (over y), dp: 2 (over x).
Axes of the slice: x: 2, y: 2, z: 4, core: 2. Of those that a mesh axis runs over, the one named last changes fastest.
Arguments:
- query_latent: bfloat16 [2, 2048, 1536], P('dp', 'seq', 'tp'), may hold values from -6 to 6
- key_latent: bfloat16 [2, 2048, 512], P('dp', 'seq', 'tp'), may hold values from -6 to 6
- rope_key: bfloat16 [2, 2048, 64], P('dp', 'seq'), may hold values from -6 to 6
- w_uq: bfloat16 [1536, 12288], P('seq', 'tp')
- w_uk: bfloat16 [512, 8192], P('seq', 'tp'), may hold values from -0.25 to 0.25
- w_uv: bfloat16 [512, 8192], P('seq', 'tp'), may hold values from -0.25 to 0.25
- block_order: int32 [2, 16], P('dp'), may hold values from 0 to 15, each once within a row
- segment_ids: int32 [2, 2048], P('dp'), may hold values from 0 to 3, never falling along the last dimension, each value on 1 to 1024 neighbouring positions
Outputs:
- context: bfloat16 [2, 2048, 8192], P('dp', 'seq', 'tp')
- clipped_uq: bfloat16 [1536, 12288], P('seq', 'tp')
- clipped_uk: bfloat16 [512, 8192], P('seq', 'tp')
The draws below stay inside these ranges and needn't reach their ends.
Inputs may be any that keep to these rules, and one draw needn't show every extreme that they name: `block_order`: each row is a permutation of the 16 position blocks. `segment_ids`: never falling along positions; each document has at most 1024 positions.
All inputs are finite; a program needn't handle non-finite values.
Results may differ from the reference program's by a relative error of at most 0.012.
The reference program's roundings to bfloat16 on the way (of `weights`) count: a program that leaves them out, or rounds other values in their place, can miss the bound.
Values may be sent and summed in bfloat16 or wider, within the bound.
A program may use at most 128 MiB of HBM per device.

```python
import math
import jax
import jax.numpy as jnp
import numpy as np
from jax import lax

HEADS = 64
NOPE = 128
ROPE = 64
VD = 128
QL = 1536
KL = 512
TOK_DEV = 256
CLIP = 8
L = 2048
BLOCKS = 16
SEQS = 2
N_DP = 2


def draw_w_uq(key, part):
    first, second = jax.random.split(jax.random.fold_in(key, 11))
    base = jax.random.normal(first, (QL, HEADS * (NOPE + ROPE)), jnp.float32) * QL ** (-0.5)
    lowest, highest = (math.log(0.5), math.log(3.0))
    exponent = jax.random.uniform(second, (HEADS,), jnp.float32, lowest, highest)
    factor = jnp.repeat(jnp.exp(exponent), NOPE + ROPE)
    return (base * factor[None, :]).astype(jnp.bfloat16)


def shard_levels(stream_key, shape, pieces, least, top_value):
    def one(axis_at, blocks):
        draws = jax.random.uniform(jax.random.fold_in(jax.random.fold_in(stream_key, 6), axis_at), (blocks,), jnp.float32, least / len(pieces), top_value / len(pieces))
        return jnp.repeat(jnp.exp(draws), shape[axis_at] // blocks).reshape((-1,) + (1,) * (len(shape) - axis_at - 1))

    level = one(*pieces[0])
    for cut in pieces[1:]:
        level = level * one(*cut)
    return level


def length_profile(amount, total, reach, slope):
    portions = [(1 << 20) // math.isqrt(rank ** slope) + 1 for rank in range(2, amount + 1)]
    rest, counts = total - reach - (amount - 1), [1] * (amount - 1)
    while rest > 0:
        free = [i for i in range(amount - 1) if counts[i] < reach]
        pool, remaining = sum([portions[i] for i in free]), rest
        for i in free:
            extra = min(reach - counts[i], max(1, remaining * portions[i] // pool), rest)
            counts[i] = counts[i] + extra
            rest = rest - extra
    return np.array([reach] + counts)


def ragged(own_key, number_of, total, limit, slope):
    if number_of == 2:
        one = jax.random.randint(own_key, (), max(1, total - limit), min(limit, total - 1) + 1)
        return jnp.stack([one, total - one])
    lengths = jnp.asarray(length_profile(number_of, total, limit, slope), jnp.int32)
    twos = (number_of - 1) // 2
    giver, taker = lengths[1:1 + 2 * twos:2], lengths[2:2 + 2 * twos:2]
    room = jnp.minimum(giver - 1, limit - taker)
    moved = jax.random.randint(jax.random.fold_in(own_key, 1), (twos,), 0, 1 << 20) % (room + 1)
    lengths = lengths.at[1:1 + 2 * twos:2].set(giver - moved).at[2:2 + 2 * twos:2].set(taker + moved)
    return lengths[jax.random.permutation(jax.random.fold_in(own_key, 2), number_of)]


def centred(rng, extent, deviation, bound, cuts=(), kind=jnp.bfloat16):
    level = shard_levels(rng, extent, cuts, -0.22, 0.18) if cuts else 1.0
    drawn = jax.random.normal(rng, extent, jnp.float32) * deviation * level
    return jnp.minimum(jnp.maximum(drawn, -bound), bound).astype(kind)


def setup_inputs(seed: int = 0) -> dict:
    splits = jax.random.split(jax.random.key(seed), 9)
    query_latent = centred(splits[0], (SEQS, L, QL), 1.0, 6.0, ((0, 2), (1, 8), (2, 2)))
    key_latent = centred(splits[1], (SEQS, L, KL), 1.0, 6.0, ((0, 2), (1, 8), (2, 2)))
    rope_key = centred(splits[2], (SEQS, L, ROPE), 1.0, 6.0, ((0, 2), (1, 8)))
    w_uq = draw_w_uq(jax.random.fold_in(splits[8], 71), 0)
    w_uk = centred(splits[4], (KL, HEADS * NOPE), KL ** -0.5, 0.25, ((0, 8), (1, 2)))
    w_uv = centred(splits[5], (KL, HEADS * VD), KL ** -0.5, 0.25, ((0, 8), (1, 2)))
    block_order = jax.vmap(lambda own: jax.random.permutation(own, BLOCKS))(jax.random.split(splits[6], SEQS)).reshape((SEQS, BLOCKS)).astype(jnp.int32)
    segment_ids = jax.vmap(lambda own: jnp.searchsorted(jnp.cumsum(ragged(own, 4, L, L // 2, 1)), jnp.arange(L), side="right"))(jax.random.split(splits[7], SEQS)).reshape((SEQS, L)).astype(jnp.int32)
    return {"query_latent": query_latent, "key_latent": key_latent, "rope_key": rope_key, "w_uq": w_uq, "w_uk": w_uk, "w_uv": w_uv, "block_order": block_order, "segment_ids": segment_ids}


rope_base = 50000.0
masked_value = -1e+30

def turning(positions, width):
    steps = jnp.arange(width // 2, dtype=jnp.float32) * (2.0 / width)
    freqs = jnp.exp(-math.log(rope_base) * steps)
    angle = positions.astype(jnp.float32)[:, None] * freqs[None, :]
    return (jnp.cos(angle), jnp.sin(angle))

def rotate(values, cosine, sine):
    half = values.shape[-1] // 2
    first = values[..., :half]
    second = values[..., half:]
    return jnp.concatenate([first * cosine - second * sine, second * cosine + first * sine], axis=-1)

def stored_positions(order, half_block):
    count = order.shape[0] * half_block
    index = jnp.arange(count, dtype=jnp.int32)
    return (jnp.take(order, index // half_block) * half_block + index % half_block).astype(jnp.int32)

def reference(query_latent, key_latent, rope_key, w_uq, w_uk, w_uv, block_order, segment_ids):
    half_block = TOK_DEV // 2
    scale = 1.0 / math.sqrt(NOPE + ROPE)
    contexts = []
    largest = jnp.full((HEADS,), masked_value, jnp.float32)
    for member in range(N_DP):
        positions = stored_positions(block_order[member], half_block)
        labels = jnp.take(segment_ids[member], positions)
        cosine, sine = turning(positions, ROPE)
        query_full = jnp.dot(query_latent[member], w_uq, preferred_element_type=jnp.float32).reshape(L, HEADS, NOPE + ROPE)
        query_nope = query_full[:, :, :NOPE].astype(jnp.bfloat16)
        query_rope = rotate(query_full[:, :, NOPE:], cosine[:, None, :], sine[:, None, :]).astype(jnp.bfloat16)
        key_nope = jnp.dot(key_latent[member], w_uk, preferred_element_type=jnp.float32).astype(jnp.bfloat16).reshape(L, HEADS, NOPE)
        values = jnp.dot(key_latent[member], w_uv, preferred_element_type=jnp.float32).astype(jnp.bfloat16).reshape(L, HEADS, VD)
        key_rope = rotate(rope_key[member].astype(jnp.float32), cosine, sine).astype(jnp.bfloat16)
        allowed = (positions[None, :] <= positions[:, None]) & (labels[None, :] == labels[:, None])

        def one_head(inputs):
            head_qn, head_qr, head_kn, head_values = inputs
            scores = jnp.dot(head_qn, head_kn.T, preferred_element_type=jnp.float32)
            scores = (scores + jnp.dot(head_qr, key_rope.T, preferred_element_type=jnp.float32)) * scale
            masked = jnp.where(allowed, scores, masked_value)
            row_max = lax.optimization_barrier(jnp.max(masked, axis=1))
            weights = jnp.where(allowed, jnp.exp(masked - row_max[:, None]), 0.0)
            total = lax.optimization_barrier(jnp.sum(weights, axis=1))
            mixed = jnp.dot(weights.astype(jnp.bfloat16), head_values, preferred_element_type=jnp.float32)
            return ((mixed / total[:, None]).astype(jnp.bfloat16), jnp.max(row_max))
        per_head, head_max = lax.map(one_head, (jnp.transpose(query_nope, (1, 0, 2)), jnp.transpose(query_rope, (1, 0, 2)), jnp.transpose(key_nope, (1, 0, 2)), jnp.transpose(values, (1, 0, 2))))
        contexts.append(jnp.transpose(per_head, (1, 0, 2)).reshape(L, HEADS * VD))
        largest = jnp.maximum(largest, head_max)
    ratio = CLIP / jnp.maximum(largest, CLIP)
    root = jnp.sqrt(ratio)
    factors = jnp.concatenate([jnp.broadcast_to(root[:, None], (HEADS, NOPE)), jnp.broadcast_to(ratio[:, None], (HEADS, ROPE))], axis=1).reshape(HEADS * (NOPE + ROPE))
    clipped_uq = (w_uq.astype(jnp.float32) * factors[None, :]).astype(jnp.bfloat16)
    clipped_uk = (w_uk.astype(jnp.float32) * jnp.repeat(root, NOPE)[None, :]).astype(jnp.bfloat16)
    return (jnp.stack(contexts), clipped_uq, clipped_uk)
```

```python
import functools
import math

import jax
import jax.numpy as jnp
import numpy as np
from jax import lax
from jax.experimental import pallas as pl
from jax.experimental.pallas import tpu as pltpu
from jax.sharding import PartitionSpec as P

NOPE = 128
ROPE = 64
VD = 128
CLIP = 8


rope_base = 50000.0
masked_value = -1e30


def turning(positions, width):
    steps = jnp.arange(width // 2, dtype=jnp.float32) * (2.0 / width)
    freqs = jnp.exp(-math.log(rope_base) * steps)
    angle = positions.astype(jnp.float32)[:, None] * freqs[None, :]
    return (jnp.cos(angle), jnp.sin(angle))


def rotate(values, cosine, sine):
    half = values.shape[-1] // 2
    first = values[..., :half]
    second = values[..., half:]
    return jnp.concatenate(
        [first * cosine - second * sine, second * cosine + first * sine], axis=-1
    )


def positions_of(index, order, half_block):
    which = index // half_block
    onehot = which[:, None] == jnp.arange(order.shape[0], dtype=jnp.int32)[None, :]
    base = jnp.sum(jnp.where(onehot, order[None, :], 0), axis=1)
    return base * half_block + index % half_block


def by_tokens(query_latent, key_latent, rope_key, w_uq, w_uk, w_uv, block_order, segment_ids):
    query_local, key_local = (
        lax.all_gather(query_latent[0], "tp", axis=1, tiled=True),
        lax.all_gather(key_latent[0], "tp", axis=1, tiled=True),
    )
    rows_uq, rows_uk, rows_uv = (
        lax.all_gather(w_uq, "seq", axis=0, tiled=True),
        lax.all_gather(w_uk, "seq", axis=0, tiled=True),
        lax.all_gather(w_uv, "seq", axis=0, tiled=True),
    )
    tok_rows = query_local.shape[0]
    half_block = tok_rows // 2
    order = block_order[0]
    labels_all = segment_ids[0]
    heads = w_uq.shape[1] // (NOPE + ROPE)
    scale = 1.0 / math.sqrt(NOPE + ROPE)
    own_index = lax.axis_index("seq") * tok_rows + jnp.arange(tok_rows, dtype=jnp.int32)
    query_pos = positions_of(own_index, order, half_block)
    query_labels = jnp.take(labels_all, query_pos)
    cosine, sine = turning(query_pos, ROPE)
    query_full = jnp.dot(query_local, rows_uq, preferred_element_type=jnp.float32).reshape(
        tok_rows, heads, NOPE + ROPE
    )
    query_nope = jnp.transpose(query_full[:, :, :NOPE].astype(jnp.bfloat16), (1, 0, 2))
    query_rope = jnp.transpose(
        rotate(query_full[:, :, NOPE:], cosine[:, None, :], sine[:, None, :]).astype(jnp.bfloat16),
        (1, 0, 2),
    )
    key_rope = rotate(rope_key[0].astype(jnp.float32), cosine, sine).astype(jnp.bfloat16)

    def slice_latent(pieces, first, width):
        latent_block = lax.dynamic_slice_in_dim(pieces[0], first, width, 0)
        rope_block = lax.dynamic_slice_in_dim(pieces[1], first, width, 0)
        nope_block = jnp.dot(latent_block, rows_uk, preferred_element_type=jnp.float32).astype(
            jnp.bfloat16
        )
        value_block = jnp.dot(latent_block, rows_uv, preferred_element_type=jnp.float32).astype(
            jnp.bfloat16
        )
        return (nope_block, value_block, rope_block)

    initial = (
        jnp.full((heads, tok_rows), masked_value, jnp.float32),
        jnp.zeros((heads, tok_rows), jnp.float32),
        jnp.zeros((heads, tok_rows, VD), jnp.float32),
    )
    pieces = (
        lax.all_gather(key_local, "seq", axis=0, tiled=True),
        lax.all_gather(key_rope, "seq", axis=0, tiled=True),
    )
    count = pieces[-1].shape[0]
    width = math.gcd(count, 512)

    def block_step(state, number):
        first = number * width
        nope_block, value_block, rope_block = slice_latent(pieces, first, width)
        nope_block = nope_block.reshape(width, heads, NOPE)
        value_block = value_block.reshape(width, heads, VD)
        key_index = first + jnp.arange(width, dtype=jnp.int32)
        key_pos = positions_of(key_index, order, half_block)
        key_labels = jnp.take(labels_all, key_pos)
        allowed = (key_pos[None, :] <= query_pos[:, None]) & (
            key_labels[None, :] == query_labels[:, None]
        )
        scores = jnp.einsum(
            "hqd,khd->hqk", query_nope, nope_block, preferred_element_type=jnp.float32
        )
        scores = (
            scores
            + jnp.einsum("hqr,kr->hqk", query_rope, rope_block, preferred_element_type=jnp.float32)
        ) * scale
        masked = jnp.where(allowed[None], scores, masked_value)
        run_max, run_total, run_sum = state
        new_max = jnp.maximum(run_max, jnp.max(masked, axis=2))
        weights = jnp.where(allowed[None], jnp.exp(masked - new_max[:, :, None]), 0.0)
        shrink = jnp.exp(run_max - new_max)
        new_total = run_total * shrink + jnp.sum(weights, axis=2)
        mixed = jnp.einsum(
            "hqk,khv->hqv",
            weights.astype(jnp.bfloat16),
            value_block,
            preferred_element_type=jnp.float32,
        )
        new_sum = run_sum * shrink[:, :, None] + mixed
        return ((new_max, new_total, new_sum), None)

    result, unused = lax.scan(block_step, initial, jnp.arange(count // width, dtype=jnp.int32))
    run_max, run_total, run_sum = result
    context = (run_sum / run_total[:, :, None]).astype(jnp.bfloat16)
    context = jnp.transpose(context, (1, 0, 2)).reshape(1, tok_rows, heads * VD)
    head_max = lax.pmax(jnp.max(run_max, axis=1), ("seq", "dp"))
    ratio = CLIP / jnp.maximum(head_max, CLIP)
    root = jnp.sqrt(ratio)
    factors = jnp.concatenate(
        [
            jnp.broadcast_to(root[:, None], (heads, NOPE)),
            jnp.broadcast_to(ratio[:, None], (heads, ROPE)),
        ],
        axis=1,
    ).reshape(heads * (NOPE + ROPE))
    clipped_uq = (w_uq.astype(jnp.float32) * factors[None, :]).astype(jnp.bfloat16)
    clipped_uk = (w_uk.astype(jnp.float32) * jnp.repeat(root, NOPE)[None, :]).astype(jnp.bfloat16)
    return (context, clipped_uq, clipped_uk)


def turned(values, cosine, sine):
    half = values.shape[-1] // 2
    swapped = jnp.concatenate([values[:, half:], values[:, :half]], axis=1)
    return values * cosine + swapped * sine


MESH = pl.DeviceIdType.MESH


def window(start, size):
    return pl.ds(pl.multiple_of(start * size, size), size)


def greet(wheres):
    barrier = pltpu.get_barrier_semaphore()
    for where in wheres:
        pl.semaphore_signal(barrier, inc=1, device_id=where, device_id_type=MESH)
    pl.semaphore_wait(barrier, len(wheres))


def fused(
    n, block, groups,
    order, inv_s, label_ref, query_ref, key_ref, rope_ref, uq_ref, uk_ref, uv_ref, turn_ref,
    out_ref, peaks_ref,
    q_lat, k_lat, r_lat, r_blk, wq_s, wk_s, wv_s, wvt_s, q_s, k_s, vt_s, s_s, p_s, c_s, lab_s, turn_s,
    peak_s,
    got_q, got_k, got_r, got_w, got_c, got_p,
    sent_l, sent_w, sent_x, sent_m, sent_c, sent_p, local_l, local_w, local_c,
):
    s, t, d = lax.axis_index("seq"), lax.axis_index("tp"), lax.axis_index("dp")
    quarter = n // 2
    level, core = s // 2, lax.rem(s, 2)
    half = s // quarter
    place = lax.rem(s, quarter)
    first_of_half = half * quarter
    mate = s + 1 - 2 * core
    pair = first_of_half + lax.rem(place + 2, quarter)
    inner = (level == quarter // 2 - 1) | (level == quarter // 2)
    gate = jnp.where(half == 0, quarter, quarter - 2) + core
    far = [(1 - half) * quarter + 2 * k + core for k in range(2)]
    others = [lax.rem(s + k, n) for k in range(1, n)]
    to_mate, to_pair, to_gate = {"seq": mate}, {"seq": pair}, {"seq": gate}
    beside, across = {"tp": 1 - t}, {"dp": 1 - d}
    peers = [{"seq": to} for to in others] + [across] + [{"seq": to, "dp": 1 - d} for to in others]
    greet(peers + [beside])

    rows, wide = query_ref.shape
    part, unused, thin = key_ref.shape
    blocks = k_lat.shape[0]
    count = blocks * block
    own_blocks = blocks // 2
    back = blocks // 2
    scale = 1.0 / math.sqrt(NOPE + ROPE)
    turn_width = NOPE + ROPE

    def link(source, target, arrived, where, sender):
        return pltpu.make_async_remote_copy(
            src_ref=source, dst_ref=target, send_sem=sender, recv_sem=arrived,
            device_id=where, device_id_type=MESH,
        )

    def arrive(target, arrived):
        link(target, target, arrived, beside, sent_l.at[0]).wait_recv()

    started = []

    def send(source, spot, where, condition=None):
        target, arrived = spot
        copy = link(source, target, arrived, where, sent_l.at[len(started)])
        if condition is None:
            copy.start()
        else:
            pl.when(condition)(copy.start)
        started.append((copy, condition))

    def q_spot(src, tp):
        at = lax.rem(src, quarter)
        return (q_lat.at[window(at, rows), window(tp, wide)], got_q.at[at, tp])

    def k_spot(src, tp):
        return (k_lat.at[window(src, part), :, window(tp, thin)], got_k.at[src, tp])

    def r_spot(src):
        return (r_lat.at[:, window(src, rows)], got_r.at[src])

    for where in (to_gate, to_pair):
        send(key_ref, k_spot(s, t), where)
        send(rope_ref, r_spot(s), where)
    send(query_ref, q_spot(s, t), to_pair)
    send(key_ref, k_spot(s, t), beside)
    send(query_ref, q_spot(s, t), beside)
    send(key_ref, k_spot(s, t), to_mate)
    send(rope_ref, r_spot(s), to_mate)
    send(query_ref, q_spot(s, t), to_mate)

    weights = ((uq_ref, wq_s), (uk_ref, wk_s), (uv_ref, wv_s))

    def w_spot(g, index, src):
        ref, held = weights[index]
        return (held.at[g, window(src, ref.shape[0]), :], got_w.at[g, index, src])

    def w_piece(g, index, to):
        ref, held = weights[index]
        return ref.at[:, window(lax.rem(to, quarter) * groups + g, held.shape[2])]

    def w_copy(g, index, slot, to):
        target, arrived = w_spot(g, index, s)
        return link(w_piece(g, index, to), target, arrived, {"seq": to}, sent_w.at[g, index, slot])

    far_to = [(1 - half) * quarter + k for k in range(quarter)]
    pair_chip = pair - core
    near_to = [pair_chip, pair_chip + 1]
    sender = core == d

    def far_copies(g):
        return [w_copy(g, i, k, to) for k, to in enumerate(far_to) for i in range(3)]

    def near_copies(g):
        return [w_copy(g, i, quarter + k, to) for k, to in enumerate(near_to) for i in range(3)]

    def start_all(copies):
        for copy in copies:
            copy.start()

    def first_weights(g, unused):
        start_all(far_copies(g))
        pl.when((g == 0) | ~inner)(lambda: start_all(near_copies(g)))
        return unused

    @pl.when(sender)
    def _():
        lax.fori_loop(0, groups, first_weights, 0)


    def mate_copies(g):
        out = []
        for i in range(3):
            target, arrived = w_spot(g, i, s)
            out.append(link(w_piece(g, i, mate), target, arrived, to_mate, sent_m.at[g, i]))
        return out

    def kept_weights(g):
        return [
            pltpu.make_async_copy(w_piece(g, i, s), w_spot(g, i, s)[0], local_w.at[g, i])
            for i in range(3)
        ]

    def near_weights(g, unused):
        start_all(kept_weights(g))
        start_all(mate_copies(g))
        return unused

    lax.fori_loop(0, groups, near_weights, 0)

    kept = [
        pltpu.make_async_copy(key_ref, k_spot(s, t)[0], local_l.at[0]),
        pltpu.make_async_copy(rope_ref, r_spot(s)[0], local_l.at[1]),
        pltpu.make_async_copy(query_ref, q_spot(s, t)[0], local_l.at[2]),
        pltpu.make_async_copy(turn_ref, turn_s, local_l.at[3]),
    ]
    start_all(kept)

    def label_step(p, unused):
        lab_s[back + p] = jnp.transpose(jnp.broadcast_to(label_ref[p], (block, block)))
        return unused

    lax.fori_loop(0, blocks, label_step, 0)

    def empty_step(p, unused):
        lab_s[p] = jnp.full((block, block), -1, jnp.int32)
        for head in range(2):
            k_s[head, p] = jnp.zeros((block, turn_width), jnp.bfloat16)
        vt_s[p] = jnp.zeros((2 * VD, block), jnp.bfloat16)
        return unused

    lax.fori_loop(0, back, empty_step, 0)

    def pass_keys(src, onward):
        arrive(*k_spot(src, t))
        arrive(*r_spot(src))
        if onward:
            send(k_spot(src, t)[0], k_spot(src, t), to_pair, inner)
            send(r_spot(src)[0], r_spot(src), to_pair, inner)
        send(k_spot(src, t)[0], k_spot(src, t), beside)
        send(k_spot(src, t)[0], k_spot(src, t), to_mate)
        send(r_spot(src)[0], r_spot(src), to_mate)

    def hand_keys(src):
        arrive(*k_spot(src, 1 - t))
        send(k_spot(src, 1 - t)[0], k_spot(src, 1 - t), to_mate)

    def hand_query(src):
        arrive(*q_spot(src, 1 - t))
        send(q_spot(src, 1 - t)[0], q_spot(src, 1 - t), to_mate)

    pass_keys(pair, False)
    for src in far:
        pass_keys(src, True)

    def later_weights(g, unused):
        start_all(near_copies(g))
        return unused

    @pl.when(sender & inner)
    def _():
        lax.fori_loop(1, groups, later_weights, 0)

    arrive(*q_spot(pair, t))
    send(q_spot(pair, t)[0], q_spot(pair, t), beside)
    send(q_spot(pair, t)[0], q_spot(pair, t), to_mate)
    hand_keys(s)
    hand_query(s)
    hand_keys(pair)
    for src in far:
        hand_keys(src)
    hand_query(pair)

    across_from = [lax.rem(level + k, quarter) * 2 for k in range(1, quarter)]

    def forward(g, k):
        src = across_from[k] + d
        for i in range(3):
            target, arrived = w_spot(g, i, src)
            arrive(target, arrived)
            link(target, target, arrived, across, sent_x.at[g, i, k]).start()

    for k in range(len(across_from)):
        forward(0, k)

    parity = 1 - core
    for src in (mate, pair + 1 - 2 * core):
        arrive(*q_spot(src, t))
        arrive(*q_spot(src, 1 - t))
    for k in range(quarter):
        src = 2 * k + parity
        arrive(*k_spot(src, t))
        arrive(*k_spot(src, 1 - t))
        arrive(*r_spot(src))
    for copy in kept:
        copy.wait()

    for b in range(blocks):
        r_blk[b] = r_lat[:, b * block : (b + 1) * block]

    def rope_step(p, unused):
        raw = jnp.transpose(r_blk[inv_s[p]].astype(jnp.float32))
        turned_key = turned(raw, turn_s[p, :, :ROPE], turn_s[p, :, ROPE:]).astype(jnp.bfloat16)
        for head in range(2):
            k_s[head, p + back, :, NOPE:] = turned_key
        return unused

    lax.fori_loop(0, blocks, rope_step, 0)

    step_blocks = 4
    chunk = step_blocks * block
    factor = scale * math.log2(math.e)

    def out_spot(g, src):
        at = lax.rem(src, quarter)
        return (out_ref.at[:, window(at * groups + g, 2 * VD)], got_c.at[g, at])

    def context_copies(g):
        out = []
        for k in range(1, quarter):
            at = lax.rem(place + k, quarter)
            target, arrived = out_spot(g, s)
            out.append(
                link(
                    c_s.at[g, window(at, rows), :], target, arrived,
                    {"seq": first_of_half + at}, sent_c.at[g, k - 1],
                )
            )
        return out

    def kept_context(g):
        return pltpu.make_async_copy(
            c_s.at[g, window(place, rows), :], out_spot(g, s)[0], local_c.at[g]
        )

    def group(g, unused):
        for k in range(len(across_from)):
            for i in range(3):
                arrive(*w_spot(g, i, across_from[k] + 1 - d))
        for i in range(3):
            arrive(*w_spot(g, i, mate))
        for copy in kept_weights(g):
            copy.wait()

        wvt_s[...] = jnp.transpose(wv_s[g])

        def keys(step, unused):
            latent = jnp.concatenate(
                [k_lat[inv_s[step * step_blocks + j]] for j in range(step_blocks)], axis=0
            )
            nope = jnp.dot(latent, wk_s[g], preferred_element_type=jnp.float32)
            nope = nope.astype(jnp.bfloat16)
            value = lax.dot_general(
                wvt_s[...], latent, (((1,), (1,)), ((), ())), preferred_element_type=jnp.float32
            )
            value = value.astype(jnp.bfloat16)
            for j in range(step_blocks):
                at, lo, hi = back + step * step_blocks + j, j * block, (j + 1) * block
                for head in range(2):
                    k_s[head, at, :, :NOPE] = nope[lo:hi, head * NOPE : (head + 1) * NOPE]
                vt_s[at] = value[:, lo:hi]
            return unused

        lax.fori_loop(0, blocks // step_blocks, keys, 0)

        def queries(step, unused):
            full = jnp.dot(
                q_lat[window(step, chunk), :], wq_s[g], preferred_element_type=jnp.float32
            )
            for j in range(step_blocks):
                b = step * step_blocks + j
                turns = turn_s[order[half * own_blocks + b]]
                cosine, sine = turns[:, :ROPE], turns[:, ROPE:]
                lo, hi = j * block, (j + 1) * block
                here = window(b, block)
                for head in range(2):
                    base = head * turn_width
                    q_s[head, here, :NOPE] = full[lo:hi, base : base + NOPE].astype(jnp.bfloat16)
                    q_s[head, here, NOPE:] = turned(
                        full[lo:hi, base + NOPE : base + turn_width], cosine, sine
                    ).astype(jnp.bfloat16)
            return unused

        lax.fori_loop(0, own_blocks // step_blocks, queries, 0)

        def attend(b, best):
            for k in range(len(across_from)):
                pl.when((b == 2 * k) & (g + 1 < groups))(lambda k=k: forward(g + 1, k))
            p = order[half * own_blocks + b]
            here = window(b, block)
            asking = label_ref[p]
            causal = lax.broadcasted_iota(jnp.int32, (block, block), 0) <= (
                lax.broadcasted_iota(jnp.int32, (block, block), 1)
            )
            raws = [
                lax.dot_general(
                    jnp.concatenate([k_s[head, p + j] for j in range(back + 1)], axis=0),
                    q_s[head, here, :], (((1,), (1,)), ((), ())),
                    preferred_element_type=jnp.float32,
                )
                for head in range(2)
            ]
            tops = [jnp.full((8, block), masked_value, jnp.float32) for head in range(2)]
            for j in range(back + 1):
                lo, hi = j * block, (j + 1) * block
                allowed = lab_s[p + j] == asking
                if j == back:
                    allowed = allowed & causal
                for head in range(2):
                    raw = jnp.where(allowed, raws[head][lo:hi, :], masked_value)
                    s_s[head, lo:hi, :] = raw
                    tops[head] = jnp.maximum(
                        tops[head], jnp.max(raw.reshape(block // 8, 8, block), axis=0)
                    )
            out = []
            for head in range(2):
                top = jnp.max(tops[head], axis=0, keepdims=True)
                total = jnp.zeros((8, block), jnp.float32)
                for j in range(back + 1):
                    lo, hi = j * block, (j + 1) * block
                    piece = jnp.exp2((s_s[head, lo:hi, :] - top) * factor)
                    total = total + jnp.sum(piece.reshape(block // 8, 8, block), axis=0)
                    p_s[head, lo:hi, :] = piece.astype(jnp.bfloat16)
                mixed = jnp.dot(
                    jnp.concatenate(
                        [vt_s[p + j, head * VD : (head + 1) * VD, :] for j in range(back + 1)], axis=1
                    ),
                    p_s[head],
                    preferred_element_type=jnp.float32,
                )
                done = mixed / jnp.sum(total, axis=0, keepdims=True)
                c_s[g, here, head * VD : (head + 1) * VD] = jnp.transpose(done).astype(
                    jnp.bfloat16
                )
                out.append(jnp.maximum(best[head], top))
            return tuple(out)

        low = jnp.full((1, block), masked_value, jnp.float32)
        best = lax.fori_loop(0, own_blocks, attend, (low, low))
        peak_s[g] = jnp.concatenate(best, axis=0) * scale
        start_all(context_copies(g))
        kept_context(g).start()
        return unused

    lax.fori_loop(0, groups, group, 0)

    me = d * n + s
    peak_copies = [
        link(peak_s, peaks_ref.at[me], got_p.at[me], where, sent_p.at[k])
        for k, where in enumerate(peers)
    ]
    start_all(peak_copies)
    keep_peak = pltpu.make_async_copy(peak_s, peaks_ref.at[me], local_l.at[4])
    keep_peak.start()

    def settle(g, unused):
        def far_sent():
            for copy in far_copies(g) + near_copies(g):
                copy.wait_send()

        pl.when(sender)(far_sent)
        for copy in mate_copies(g):
            copy.wait_send()
        for k in range(len(across_from)):
            for i in range(3):
                target, arrived = w_spot(g, i, across_from[k] + d)
                link(target, target, arrived, across, sent_x.at[g, i, k]).wait_send()
        for copy in context_copies(g):
            copy.wait_send()
        kept_context(g).wait()
        for k in range(1, quarter):
            arrive(*out_spot(g, first_of_half + lax.rem(place + k, quarter)))
        return unused

    lax.fori_loop(0, groups, settle, 0)
    for copy, condition in started:
        if condition is None:
            copy.wait_send()
        else:
            pl.when(condition)(copy.wait_send)
    for copy in peak_copies:
        copy.wait_send()
    keep_peak.wait()
    for src in [d * n + to for to in others] + [(1 - d) * n + to for to in others] + [(1 - d) * n + s]:
        arrive(peaks_ref.at[src], got_p.at[src])


def by_halves(query_latent, key_latent, rope_key, w_uq, w_uk, w_uv, block_order, segment_ids):
    devices = lax.axis_size("seq")
    sides = lax.axis_size("tp")
    heads = w_uq.shape[1] // (NOPE + ROPE)
    quarter = devices // 2
    groups = heads // quarter // 2
    rows = query_latent.shape[1]
    order, labels = block_order[0], segment_ids[0]
    count, blocks = labels.shape[0], order.shape[0]
    block = count // blocks
    back = blocks // 2
    anyplace = pl.BlockSpec(memory_space=pl.ANY)
    vmem = pl.BlockSpec(memory_space=pltpu.VMEM)
    smem = pl.BlockSpec(memory_space=pltpu.SMEM)
    steps = np.arange(ROPE // 2, dtype=np.float32) * np.float32(2.0 / ROPE)
    freqs = np.exp(np.float32(-math.log(rope_base)) * steps).astype(np.float32)
    angle = np.arange(count, dtype=np.float32)[:, None] * freqs[None, :]
    cosine, sine = np.cos(angle), np.sin(angle)
    turns = jnp.asarray(np.concatenate([cosine, cosine, -sine, sine], axis=1), jnp.float32)
    every = jnp.arange(blocks, dtype=jnp.int32)
    stored_at = jnp.sum(jnp.where(order[None, :] == every[:, None], every[None, :], 0), axis=1)
    bf, f32 = jnp.bfloat16, jnp.float32
    dma = pltpu.SemaphoreType.DMA
    context, peaks = pl.pallas_call(
        functools.partial(fused, devices, block, groups),
        out_shape=[
            jax.ShapeDtypeStruct((rows, heads * VD), bf),
            jax.ShapeDtypeStruct((2 * devices, groups, 2, block), f32),
        ],
        in_specs=[smem, smem, vmem] + [anyplace] * 7,
        out_specs=[anyplace, vmem],
        scratch_shapes=[
            pltpu.VMEM((count // 2, sides * query_latent.shape[2]), bf),
            pltpu.VMEM((blocks, block, sides * key_latent.shape[2]), bf),
            pltpu.VMEM((ROPE, count), bf),
            pltpu.VMEM((blocks, ROPE, block), bf),
            pltpu.VMEM((groups, devices * w_uq.shape[0], 2 * (NOPE + ROPE)), bf),
            pltpu.VMEM((groups, devices * w_uk.shape[0], 2 * NOPE), bf),
            pltpu.VMEM((groups, devices * w_uv.shape[0], 2 * VD), bf),
            pltpu.VMEM((2 * VD, devices * w_uv.shape[0]), bf),
            pltpu.VMEM((2, count // 2, NOPE + ROPE), bf),
            pltpu.VMEM((2, back + blocks, block, NOPE + ROPE), bf),
            pltpu.VMEM((back + blocks, 2 * VD, block), bf),
            pltpu.VMEM((2, (back + 1) * block, block), f32),
            pltpu.VMEM((2, (back + 1) * block, block), bf),
            pltpu.VMEM((groups, count // 2, 2 * VD), bf),
            pltpu.VMEM((back + blocks, block, block), jnp.int32),
            pltpu.VMEM((blocks, block, 2 * ROPE), f32),
            pltpu.VMEM((groups, 2, block), f32),
            dma((quarter, sides)),
            dma((devices, sides)),
            dma((devices,)),
            dma((groups, 3, devices)),
            dma((groups, quarter)),
            dma((2 * devices,)),
            dma((40,)),
            dma((groups, 3, quarter + 2)),
            dma((groups, 3, quarter - 1)),
            dma((groups, 3)),
            dma((groups, quarter - 1)),
            dma((2 * devices,)),
            dma((5,)),
            dma((groups, 3)),
            dma((groups,)),
        ],
        compiler_params=pltpu.CompilerParams(
            collective_id=0, has_side_effects=True, vmem_limit_bytes=60 * 1024 * 1024
        ),
        name="fused",
    )(
        order, stored_at, labels.reshape(blocks, 1, block), query_latent[0],
        key_latent[0].reshape(rows // block, block, key_latent.shape[2]),
        jnp.transpose(rope_key[0]), w_uq, w_uk, w_uv, turns.reshape(blocks, block, 2 * ROPE),
    )
    head_max = jnp.max(peaks.reshape(2, 2, heads, block), axis=(0, 1, 3))
    return (context[None],) + clipped(w_uq, w_uk, head_max, heads)


def clipped(w_uq, w_uk, head_max, heads):
    ratio = CLIP / jnp.maximum(head_max, CLIP)
    root = jnp.sqrt(ratio)
    factors = jnp.concatenate(
        [
            jnp.broadcast_to(root[:, None], (heads, NOPE)),
            jnp.broadcast_to(ratio[:, None], (heads, ROPE)),
        ],
        axis=1,
    ).reshape(heads * (NOPE + ROPE))
    clipped_uq = (w_uq.astype(jnp.float32) * factors[None, :]).astype(jnp.bfloat16)
    clipped_uk = (w_uk.astype(jnp.float32) * jnp.repeat(root, NOPE)[None, :]).astype(jnp.bfloat16)
    return (clipped_uq, clipped_uk)


def on_device(*arrays):
    heads = arrays[3].shape[1] // (NOPE + ROPE)
    pairs = lax.axis_size("tp") == 2 and lax.axis_size("dp") == 2
    if pairs and lax.axis_size("seq") == 8 and heads % 8 == 0:
        return by_halves(*arrays)
    return by_tokens(*arrays)


def solution(mesh):
    placed = (
        P("dp", "seq", "tp"),
        P("dp", "seq", "tp"),
        P("dp", "seq", None),
        P("seq", "tp"),
        P("seq", "tp"),
        P("seq", "tp"),
        P("dp", None),
        P("dp", None),
    )
    return jax.shard_map(
        on_device,
        mesh=mesh,
        in_specs=placed,
        out_specs=(P("dp", "seq", "tp"), P("seq", "tp"), P("seq", "tp")),
        check_vma=False,
    )
```

```python
import functools
import math

import jax
import jax.numpy as jnp
import numpy as np
from jax import lax
from jax.experimental import pallas as pl
from jax.experimental.pallas import tpu as pltpu
from jax.sharding import PartitionSpec as P

NOPE = 128
ROPE = 64
VD = 128
CLIP = 8


rope_base = 50000.0
masked_value = -1e30


def turning(positions, width):
    steps = jnp.arange(width // 2, dtype=jnp.float32) * (2.0 / width)
    freqs = jnp.exp(-math.log(rope_base) * steps)
    angle = positions.astype(jnp.float32)[:, None] * freqs[None, :]
    return (jnp.cos(angle), jnp.sin(angle))


def rotate(values, cosine, sine):
    half = values.shape[-1] // 2
    first = values[..., :half]
    second = values[..., half:]
    return jnp.concatenate(
        [first * cosine - second * sine, second * cosine + first * sine], axis=-1
    )


def positions_of(index, order, half_block):
    which = index // half_block
    onehot = which[:, None] == jnp.arange(order.shape[0], dtype=jnp.int32)[None, :]
    base = jnp.sum(jnp.where(onehot, order[None, :], 0), axis=1)
    return base * half_block + index % half_block


def by_tokens(query_latent, key_latent, rope_key, w_uq, w_uk, w_uv, block_order, segment_ids):
    query_local, key_local = (
        lax.all_gather(query_latent[0], "tp", axis=1, tiled=True),
        lax.all_gather(key_latent[0], "tp", axis=1, tiled=True),
    )
    rows_uq, rows_uk, rows_uv = (
        lax.all_gather(w_uq, "seq", axis=0, tiled=True),
        lax.all_gather(w_uk, "seq", axis=0, tiled=True),
        lax.all_gather(w_uv, "seq", axis=0, tiled=True),
    )
    tok_rows = query_local.shape[0]
    half_block = tok_rows // 2
    order = block_order[0]
    labels_all = segment_ids[0]
    heads = w_uq.shape[1] // (NOPE + ROPE)
    scale = 1.0 / math.sqrt(NOPE + ROPE)
    own_index = lax.axis_index("seq") * tok_rows + jnp.arange(tok_rows, dtype=jnp.int32)
    query_pos = positions_of(own_index, order, half_block)
    query_labels = jnp.take(labels_all, query_pos)
    cosine, sine = turning(query_pos, ROPE)
    query_full = jnp.dot(query_local, rows_uq, preferred_element_type=jnp.float32).reshape(
        tok_rows, heads, NOPE + ROPE
    )
    query_nope = jnp.transpose(query_full[:, :, :NOPE].astype(jnp.bfloat16), (1, 0, 2))
    query_rope = jnp.transpose(
        rotate(query_full[:, :, NOPE:], cosine[:, None, :], sine[:, None, :]).astype(jnp.bfloat16),
        (1, 0, 2),
    )
    key_rope = rotate(rope_key[0].astype(jnp.float32), cosine, sine).astype(jnp.bfloat16)

    def slice_latent(pieces, first, width):
        latent_block = lax.dynamic_slice_in_dim(pieces[0], first, width, 0)
        rope_block = lax.dynamic_slice_in_dim(pieces[1], first, width, 0)
        nope_block = jnp.dot(latent_block, rows_uk, preferred_element_type=jnp.float32).astype(
            jnp.bfloat16
        )
        value_block = jnp.dot(latent_block, rows_uv, preferred_element_type=jnp.float32).astype(
            jnp.bfloat16
        )
        return (nope_block, value_block, rope_block)

    initial = (
        jnp.full((heads, tok_rows), masked_value, jnp.float32),
        jnp.zeros((heads, tok_rows), jnp.float32),
        jnp.zeros((heads, tok_rows, VD), jnp.float32),
    )
    pieces = (
        lax.all_gather(key_local, "seq", axis=0, tiled=True),
        lax.all_gather(key_rope, "seq", axis=0, tiled=True),
    )
    count = pieces[-1].shape[0]
    width = math.gcd(count, 512)

    def block_step(state, number):
        first = number * width
        nope_block, value_block, rope_block = slice_latent(pieces, first, width)
        nope_block = nope_block.reshape(width, heads, NOPE)
        value_block = value_block.reshape(width, heads, VD)
        key_index = first + jnp.arange(width, dtype=jnp.int32)
        key_pos = positions_of(key_index, order, half_block)
        key_labels = jnp.take(labels_all, key_pos)
        allowed = (key_pos[None, :] <= query_pos[:, None]) & (
            key_labels[None, :] == query_labels[:, None]
        )
        scores = jnp.einsum(
            "hqd,khd->hqk", query_nope, nope_block, preferred_element_type=jnp.float32
        )
        scores = (
            scores
            + jnp.einsum("hqr,kr->hqk", query_rope, rope_block, preferred_element_type=jnp.float32)
        ) * scale
        masked = jnp.where(allowed[None], scores, masked_value)
        run_max, run_total, run_sum = state
        new_max = jnp.maximum(run_max, jnp.max(masked, axis=2))
        weights = jnp.where(allowed[None], jnp.exp(masked - new_max[:, :, None]), 0.0)
        shrink = jnp.exp(run_max - new_max)
        new_total = run_total * shrink + jnp.sum(weights, axis=2)
        mixed = jnp.einsum(
            "hqk,khv->hqv",
            weights.astype(jnp.bfloat16),
            value_block,
            preferred_element_type=jnp.float32,
        )
        new_sum = run_sum * shrink[:, :, None] + mixed
        return ((new_max, new_total, new_sum), None)

    result, unused = lax.scan(block_step, initial, jnp.arange(count // width, dtype=jnp.int32))
    run_max, run_total, run_sum = result
    context = (run_sum / run_total[:, :, None]).astype(jnp.bfloat16)
    context = jnp.transpose(context, (1, 0, 2)).reshape(1, tok_rows, heads * VD)
    head_max = lax.pmax(jnp.max(run_max, axis=1), ("seq", "dp"))
    ratio = CLIP / jnp.maximum(head_max, CLIP)
    root = jnp.sqrt(ratio)
    factors = jnp.concatenate(
        [
            jnp.broadcast_to(root[:, None], (heads, NOPE)),
            jnp.broadcast_to(ratio[:, None], (heads, ROPE)),
        ],
        axis=1,
    ).reshape(heads * (NOPE + ROPE))
    clipped_uq = (w_uq.astype(jnp.float32) * factors[None, :]).astype(jnp.bfloat16)
    clipped_uk = (w_uk.astype(jnp.float32) * jnp.repeat(root, NOPE)[None, :]).astype(jnp.bfloat16)
    return (context, clipped_uq, clipped_uk)


def turned(values, cosine, sine):
    half = values.shape[-1] // 2
    swapped = jnp.concatenate([values[:, half:], values[:, :half]], axis=1)
    return values * cosine + swapped * sine


MESH = pl.DeviceIdType.MESH


def window(start, size):
    return pl.ds(pl.multiple_of(start * size, size), size)


def greet(wheres):
    barrier = pltpu.get_barrier_semaphore()
    for where in wheres:
        pl.semaphore_signal(barrier, inc=1, device_id=where, device_id_type=MESH)
    pl.semaphore_wait(barrier, len(wheres))


def fused(
    n, block, groups,
    order, label_ref, query_ref, key_ref, rope_ref, uq_ref, uk_ref, uv_ref, turn_ref,
    out_ref, peaks_ref,
    q_lat, k_lat, r_lat, r_blk, wq_s, wk_s, wv_s, wvt_s, q_s, k_s, vt_s, s_s, p_s, c_s, lab_s, turn_s,
    peak_s, inv_s,
    got_q, got_k, got_r, got_w, got_c, got_p,
    sent_l, sent_w, sent_x, sent_m, sent_c, sent_p, local_l, local_w, local_c,
):
    s, t, d = lax.axis_index("seq"), lax.axis_index("tp"), lax.axis_index("dp")
    quarter = n // 2
    level, core = s // 2, lax.rem(s, 2)
    half = s // quarter
    place = lax.rem(s, quarter)
    first_of_half = half * quarter
    mate = s + 1 - 2 * core
    pair = first_of_half + lax.rem(place + 2, quarter)
    inner = (level == quarter // 2 - 1) | (level == quarter // 2)
    gate = jnp.where(half == 0, quarter, quarter - 2) + core
    far = [(1 - half) * quarter + 2 * k + core for k in range(2)]
    others = [lax.rem(s + k, n) for k in range(1, n)]
    to_mate, to_pair, to_gate = {"seq": mate}, {"seq": pair}, {"seq": gate}
    beside, across = {"tp": 1 - t}, {"dp": 1 - d}
    peers = [{"seq": to} for to in others] + [across] + [{"seq": to, "dp": 1 - d} for to in others]
    greet(peers + [beside])

    rows, wide = query_ref.shape
    part, unused, thin = key_ref.shape
    blocks = k_lat.shape[0]
    count = blocks * block
    own_blocks = blocks // 2
    back = blocks // 2
    scale = 1.0 / math.sqrt(NOPE + ROPE)
    turn_width = NOPE + ROPE

    def link(source, target, arrived, where, sender):
        return pltpu.make_async_remote_copy(
            src_ref=source, dst_ref=target, send_sem=sender, recv_sem=arrived,
            device_id=where, device_id_type=MESH,
        )

    def arrive(target, arrived):
        link(target, target, arrived, beside, sent_l.at[0]).wait_recv()

    started = []
    state = {"when": None}

    def send(source, spot, where):
        target, arrived = spot()
        source = target if source is None else source
        link(source, target, arrived, where, sent_l.at[len(started)]).start()
        started.append((spot, where, state["when"]))

    def under(condition, action):
        state["when"] = condition
        pl.when(condition)(action)
        state["when"] = None

    def q_spot(src, tp):
        at = lax.rem(src, quarter)
        return (q_lat.at[window(at, rows), window(tp, wide)], got_q.at[at, tp])

    def k_spot(src, tp):
        return (k_lat.at[window(src, part), :, window(tp, thin)], got_k.at[src, tp])

    def r_spot(src):
        return (r_lat.at[:, window(src, rows)], got_r.at[src])

    for where in (to_gate, to_pair):
        send(key_ref, lambda: k_spot(s, t), where)
        send(rope_ref, lambda: r_spot(s), where)
    send(query_ref, lambda: q_spot(s, t), to_pair)
    send(key_ref, lambda: k_spot(s, t), beside)
    send(query_ref, lambda: q_spot(s, t), beside)
    send(key_ref, lambda: k_spot(s, t), to_mate)
    send(rope_ref, lambda: r_spot(s), to_mate)
    send(query_ref, lambda: q_spot(s, t), to_mate)

    weights = ((uk_ref, wk_s), (uv_ref, wv_s), (uq_ref, wq_s))

    def w_spot(g, index, src):
        ref, held = weights[index]
        return (held.at[g, window(src, ref.shape[0]), :], got_w.at[g, index, src])

    def w_piece(g, index, to):
        ref, held = weights[index]
        return ref.at[:, window(lax.rem(to, quarter) * groups + g, held.shape[2])]

    def w_copy(g, index, slot, to):
        target, arrived = w_spot(g, index, s)
        return link(w_piece(g, index, to), target, arrived, {"seq": to}, sent_w.at[g, index, slot])

    far_to = [
        (1 - half) * quarter + lax.rem(k + 2 * lax.rem(level, 2), quarter) for k in range(quarter)
    ]
    pair_chip = pair - core
    near_to = [pair_chip, pair_chip + 1]
    sender = core == d

    def far_copies(g):
        return [w_copy(g, i, k, to) for k, to in enumerate(far_to) for i in range(3)]

    def near_copies(g):
        return [w_copy(g, i, quarter + k, to) for k, to in enumerate(near_to) for i in range(3)]

    def start_all(copies):
        for copy in copies:
            copy.start()

    def send_weights(g):
        start_all(near_copies(g) + far_copies(g))

    pl.when(sender & ~inner)(lambda: start_all(near_copies(0)))
    pl.when(sender)(lambda: start_all(far_copies(0)))


    def mate_copies(g):
        out = []
        for i in range(3):
            target, arrived = w_spot(g, i, s)
            out.append(link(w_piece(g, i, mate), target, arrived, to_mate, sent_m.at[g, i]))
        return out

    def kept_weights(g):
        return [
            pltpu.make_async_copy(w_piece(g, i, s), w_spot(g, i, s)[0], local_w.at[g, i])
            for i in range(3)
        ]

    def near_weights(g, unused):
        start_all(kept_weights(g))
        start_all(mate_copies(g))
        return unused

    lax.fori_loop(0, groups, near_weights, 0)

    kept = [
        pltpu.make_async_copy(key_ref, k_spot(s, t)[0], local_l.at[0]),
        pltpu.make_async_copy(rope_ref, r_spot(s)[0], local_l.at[1]),
        pltpu.make_async_copy(query_ref, q_spot(s, t)[0], local_l.at[2]),
        pltpu.make_async_copy(turn_ref, turn_s, local_l.at[3]),
    ]
    start_all(kept)

    def label_step(p, unused):
        at = 0
        for b in range(blocks):
            at = jnp.where(order[b] == p, b, at)
        inv_s[p] = at
        lab_s[back + p] = jnp.transpose(jnp.broadcast_to(label_ref[p], (block, block)))
        return unused

    lax.fori_loop(0, blocks, label_step, 0)

    def empty_step(p, unused):
        lab_s[p] = jnp.full((block, block), -1, jnp.int32)
        for head in range(2):
            k_s[head, p] = jnp.zeros((block, turn_width), jnp.bfloat16)
        vt_s[p] = jnp.zeros((2 * VD, block), jnp.bfloat16)
        return unused

    lax.fori_loop(0, back, empty_step, 0)

    def pass_keys(src, onward):
        arrive(*k_spot(src, t))
        arrive(*r_spot(src))
        if onward:
            send(None, lambda: k_spot(src, t), to_pair)
            send(None, lambda: r_spot(src), to_pair)
        send(None, lambda: k_spot(src, t), beside)
        send(None, lambda: k_spot(src, t), to_mate)
        send(None, lambda: r_spot(src), to_mate)

    def hand_keys(src):
        arrive(*k_spot(src, 1 - t))
        send(None, lambda: k_spot(src, 1 - t), to_mate)

    def hand_query(src):
        arrive(*q_spot(src, 1 - t))
        send(None, lambda: q_spot(src, 1 - t), to_mate)

    def turn_ropes():
        for b in range(blocks):
            r_blk[b] = r_lat[:, b * block : (b + 1) * block]

        def rope_step(p, unused):
            raw = jnp.transpose(r_blk[inv_s[p]].astype(jnp.float32))
            turned_key = turned(raw, turn_s[p, :, :ROPE], turn_s[p, :, ROPE:]).astype(jnp.bfloat16)
            for head in range(2):
                k_s[head, p + back, :, NOPE:] = turned_key
            return unused

        lax.fori_loop(0, blocks, rope_step, 0)

    across_from = [pair_chip, gate - core, 2 * (1 - half) * quarter + quarter - 2 - (gate - core)]

    def forward(g, k):
        src = across_from[k] + d
        for i in range(3):
            target, arrived = w_spot(g, i, src)
            arrive(target, arrived)
            link(target, target, arrived, across, sent_x.at[g, i, k]).start()

    def pass_query():
        arrive(*q_spot(pair, t))
        send(None, lambda: q_spot(pair, t), beside)
        send(None, lambda: q_spot(pair, t), to_mate)

    def relay():
        for src in far:
            pass_keys(src, True)

    def take():
        for src in far:
            pass_keys(src, False)

    pass_keys(pair, False)
    under(inner, relay)
    pl.when(sender & inner)(lambda: start_all(near_copies(0)))
    hand_keys(s)
    hand_query(s)
    pass_query()
    hand_keys(pair)
    forward(0, 1)
    pl.when(sender)(lambda: send_weights(1))
    forward(0, 2)
    under(~inner, take)
    for src in far:
        hand_keys(src)
    hand_query(pair)
    forward(0, 0)
    pl.when(sender)(lambda: send_weights(2))

    for k in range(quarter):
        src = 2 * k + 1 - core
        arrive(*k_spot(src, t))
        arrive(*k_spot(src, 1 - t))
        arrive(*r_spot(src))
    for copy in kept:
        copy.wait()
    turn_ropes()
    for src in (mate, pair + 1 - 2 * core):
        arrive(*q_spot(src, t))
        arrive(*q_spot(src, 1 - t))

    step_blocks = 4
    chunk = step_blocks * block
    factor = scale * math.log2(math.e)

    def out_spot(g, src):
        at = lax.rem(src, quarter)
        return (out_ref.at[:, window(at * groups + g, 2 * VD)], got_c.at[g, at])

    other_chip = lax.rem(place - core + 2, quarter)

    def context_to(g, k):
        at = lax.rem(other_chip + k, quarter)
        target, arrived = out_spot(g, s)
        return link(
            c_s.at[g, window(at, rows), :], target, arrived,
            {"seq": first_of_half + at}, sent_c.at[g, k],
        )

    def kept_context(g):
        return pltpu.make_async_copy(
            c_s.at[g, window(place, rows), :], out_spot(g, s)[0], local_c.at[g]
        )

    def leave(g, k):
        if k < 2:
            context_to(g, k).start()
        else:
            pl.when(core == k - 2)(kept_context(g).start)
            pl.when(core != k - 2)(context_to(g, k).start)

    def left(g):
        for k in range(2):
            context_to(g, k).wait_send()
        for k in range(2, 4):
            pl.when(core != k - 2)(context_to(g, k).wait_send)
        kept_context(g).wait()

    def group(g, unused):
        pl.when(sender & (g + 3 < groups))(lambda: send_weights(g + 3))
        for k in range(len(across_from)):
            for i in range(3):
                arrive(*w_spot(g, i, across_from[k] + 1 - d))
        for i in range(3):
            arrive(*w_spot(g, i, mate))
        for copy in kept_weights(g):
            copy.wait()

        def onward(k):
            pl.when(g + 1 < groups)(lambda: forward(g + 1, k))

        wvt_s[...] = jnp.transpose(wv_s[g])

        def keys(step, unused):
            latent = jnp.concatenate(
                [k_lat[inv_s[step * step_blocks + j]] for j in range(step_blocks)], axis=0
            )
            nope = jnp.dot(latent, wk_s[g], preferred_element_type=jnp.float32)
            nope = nope.astype(jnp.bfloat16)
            value = lax.dot_general(
                wvt_s[...], latent, (((1,), (1,)), ((), ())), preferred_element_type=jnp.float32
            )
            value = value.astype(jnp.bfloat16)
            for j in range(step_blocks):
                at, lo, hi = back + step * step_blocks + j, j * block, (j + 1) * block
                for head in range(2):
                    k_s[head, at, :, :NOPE] = nope[lo:hi, head * NOPE : (head + 1) * NOPE]
                vt_s[at] = value[:, lo:hi]
            return unused

        onward(0)
        lax.fori_loop(0, blocks // step_blocks, keys, 0)
        onward(1)

        def queries(step, unused):
            full = jnp.dot(
                q_lat[window(step, chunk), :], wq_s[g], preferred_element_type=jnp.float32
            )
            for j in range(step_blocks):
                b = step * step_blocks + j
                turns = turn_s[order[half * own_blocks + b]]
                cosine, sine = turns[:, :ROPE], turns[:, ROPE:]
                lo, hi = j * block, (j + 1) * block
                here = window(b, block)
                for head in range(2):
                    base = head * turn_width
                    q_s[head, here, :NOPE] = full[lo:hi, base : base + NOPE].astype(jnp.bfloat16)
                    q_s[head, here, NOPE:] = turned(
                        full[lo:hi, base + NOPE : base + turn_width], cosine, sine
                    ).astype(jnp.bfloat16)
            return unused

        lax.fori_loop(0, own_blocks // step_blocks, queries, 0)
        onward(2)

        def attend(step, best):
            b = lax.rem(other_chip * part + step, own_blocks)
            p = order[half * own_blocks + b]
            here = window(b, block)
            asking = label_ref[p]
            causal = lax.broadcasted_iota(jnp.int32, (block, block), 0) <= (
                lax.broadcasted_iota(jnp.int32, (block, block), 1)
            )
            raws = [
                lax.dot_general(
                    jnp.concatenate([k_s[head, p + j] for j in range(back + 1)], axis=0),
                    q_s[head, here, :], (((1,), (1,)), ((), ())),
                    preferred_element_type=jnp.float32,
                )
                for head in range(2)
            ]
            tops = [jnp.full((8, block), masked_value, jnp.float32) for head in range(2)]
            for j in range(back + 1):
                lo, hi = j * block, (j + 1) * block
                allowed = lab_s[p + j] == asking
                if j == back:
                    allowed = allowed & causal
                for head in range(2):
                    raw = jnp.where(allowed, raws[head][lo:hi, :], masked_value)
                    s_s[head, lo:hi, :] = raw
                    tops[head] = jnp.maximum(
                        tops[head], jnp.max(raw.reshape(block // 8, 8, block), axis=0)
                    )
            out = []
            for head in range(2):
                top = jnp.max(tops[head], axis=0, keepdims=True)
                total = jnp.zeros((8, block), jnp.float32)
                for j in range(back + 1):
                    lo, hi = j * block, (j + 1) * block
                    piece = jnp.exp2((s_s[head, lo:hi, :] - top) * factor)
                    total = total + jnp.sum(piece.reshape(block // 8, 8, block), axis=0)
                    p_s[head, lo:hi, :] = piece.astype(jnp.bfloat16)
                mixed = jnp.dot(
                    jnp.concatenate(
                        [vt_s[p + j, head * VD : (head + 1) * VD, :] for j in range(back + 1)], axis=1
                    ),
                    p_s[head],
                    preferred_element_type=jnp.float32,
                )
                done = mixed / jnp.sum(total, axis=0, keepdims=True)
                c_s[g, here, head * VD : (head + 1) * VD] = jnp.transpose(done).astype(
                    jnp.bfloat16
                )
                out.append(jnp.maximum(best[head], top))
            for k in range(3):
                pl.when(step == (k + 1) * part)(lambda k=k: leave(g, k))
            return tuple(out)

        low = jnp.full((1, block), masked_value, jnp.float32)
        best = lax.fori_loop(0, own_blocks, attend, (low, low))
        peak_s[g] = jnp.concatenate(best, axis=0) * scale
        leave(g, 3)
        return unused

    lax.fori_loop(0, groups, group, 0)

    me = d * n + s
    peak_copies = [
        link(peak_s, peaks_ref.at[me], got_p.at[me], where, sent_p.at[k])
        for k, where in enumerate(peers)
    ]
    start_all(peak_copies)
    keep_peak = pltpu.make_async_copy(peak_s, peaks_ref.at[me], local_l.at[4])
    keep_peak.start()

    def settle(g, unused):
        def far_sent():
            for copy in far_copies(g) + near_copies(g):
                copy.wait_send()

        pl.when(sender)(far_sent)
        for copy in mate_copies(g):
            copy.wait_send()
        for k in range(len(across_from)):
            for i in range(3):
                target, arrived = w_spot(g, i, across_from[k] + d)
                link(target, target, arrived, across, sent_x.at[g, i, k]).wait_send()
        left(g)
        for k in range(1, quarter):
            arrive(*out_spot(g, first_of_half + lax.rem(place + k, quarter)))
        return unused

    lax.fori_loop(0, groups, settle, 0)
    for k, (spot, where, condition) in enumerate(started):
        target, arrived = spot()
        copy = link(target, target, arrived, where, sent_l.at[k])
        if condition is None:
            copy.wait_send()
        else:
            pl.when(condition)(copy.wait_send)
    for copy in peak_copies:
        copy.wait_send()
    keep_peak.wait()
    for src in [d * n + to for to in others] + [(1 - d) * n + to for to in others] + [(1 - d) * n + s]:
        arrive(peaks_ref.at[src], got_p.at[src])


def by_halves(query_latent, key_latent, rope_key, w_uq, w_uk, w_uv, block_order, segment_ids):
    devices = lax.axis_size("seq")
    sides = lax.axis_size("tp")
    heads = w_uq.shape[1] // (NOPE + ROPE)
    quarter = devices // 2
    groups = heads // quarter // 2
    rows = query_latent.shape[1]
    order, labels = block_order[0], segment_ids[0]
    count, blocks = labels.shape[0], order.shape[0]
    block = count // blocks
    back = blocks // 2
    anyplace = pl.BlockSpec(memory_space=pl.ANY)
    vmem = pl.BlockSpec(memory_space=pltpu.VMEM)
    smem = pl.BlockSpec(memory_space=pltpu.SMEM)
    steps = np.arange(ROPE // 2, dtype=np.float32) * np.float32(2.0 / ROPE)
    freqs = np.exp(np.float32(-math.log(rope_base)) * steps).astype(np.float32)
    angle = np.arange(count, dtype=np.float32)[:, None] * freqs[None, :]
    cosine, sine = np.cos(angle), np.sin(angle)
    turns = jnp.asarray(np.concatenate([cosine, cosine, -sine, sine], axis=1), jnp.float32)
    bf, f32 = jnp.bfloat16, jnp.float32
    dma = pltpu.SemaphoreType.DMA
    context, peaks = pl.pallas_call(
        functools.partial(fused, devices, block, groups),
        out_shape=[
            jax.ShapeDtypeStruct((rows, heads * VD), bf),
            jax.ShapeDtypeStruct((2 * devices, groups, 2, block), f32),
        ],
        in_specs=[smem, vmem] + [anyplace] * 7,
        out_specs=[anyplace, vmem],
        scratch_shapes=[
            pltpu.VMEM((count // 2, sides * query_latent.shape[2]), bf),
            pltpu.VMEM((blocks, block, sides * key_latent.shape[2]), bf),
            pltpu.VMEM((ROPE, count), bf),
            pltpu.VMEM((blocks, ROPE, block), bf),
            pltpu.VMEM((groups, devices * w_uq.shape[0], 2 * (NOPE + ROPE)), bf),
            pltpu.VMEM((groups, devices * w_uk.shape[0], 2 * NOPE), bf),
            pltpu.VMEM((groups, devices * w_uv.shape[0], 2 * VD), bf),
            pltpu.VMEM((2 * VD, devices * w_uv.shape[0]), bf),
            pltpu.VMEM((2, count // 2, NOPE + ROPE), bf),
            pltpu.VMEM((2, back + blocks, block, NOPE + ROPE), bf),
            pltpu.VMEM((back + blocks, 2 * VD, block), bf),
            pltpu.VMEM((2, (back + 1) * block, block), f32),
            pltpu.VMEM((2, (back + 1) * block, block), bf),
            pltpu.VMEM((groups, count // 2, 2 * VD), bf),
            pltpu.VMEM((back + blocks, block, block), jnp.int32),
            pltpu.VMEM((blocks, block, 2 * ROPE), f32),
            pltpu.VMEM((groups, 2, block), f32),
            pltpu.SMEM((blocks,), jnp.int32),
            dma((quarter, sides)),
            dma((devices, sides)),
            dma((devices,)),
            dma((groups, 3, devices)),
            dma((groups, quarter)),
            dma((2 * devices,)),
            dma((40,)),
            dma((groups, 3, quarter + 2)),
            dma((groups, 3, quarter - 1)),
            dma((groups, 3)),
            dma((groups, quarter)),
            dma((2 * devices,)),
            dma((5,)),
            dma((groups, 3)),
            dma((groups,)),
        ],
        compiler_params=pltpu.CompilerParams(
            collective_id=0, has_side_effects=True, vmem_limit_bytes=60 * 1024 * 1024
        ),
        name="fused",
    )(
        order, labels.reshape(blocks, 1, block), query_latent[0],
        key_latent[0].reshape(rows // block, block, key_latent.shape[2]),
        jnp.transpose(rope_key[0]), w_uq, w_uk, w_uv, turns.reshape(blocks, block, 2 * ROPE),
    )
    head_max = jnp.max(peaks.reshape(2, 2, heads, block), axis=(0, 1, 3))
    return (context[None],) + clipped(w_uq, w_uk, head_max, heads)


def clipped(w_uq, w_uk, head_max, heads):
    ratio = CLIP / jnp.maximum(head_max, CLIP)
    root = jnp.sqrt(ratio)
    factors = jnp.concatenate(
        [
            jnp.broadcast_to(root[:, None], (heads, NOPE)),
            jnp.broadcast_to(ratio[:, None], (heads, ROPE)),
        ],
        axis=1,
    ).reshape(heads * (NOPE + ROPE))
    clipped_uq = (w_uq.astype(jnp.float32) * factors[None, :]).astype(jnp.bfloat16)
    clipped_uk = (w_uk.astype(jnp.float32) * jnp.repeat(root, NOPE)[None, :]).astype(jnp.bfloat16)
    return (clipped_uq, clipped_uk)


def on_device(*arrays):
    heads = arrays[3].shape[1] // (NOPE + ROPE)
    pairs = lax.axis_size("tp") == 2 and lax.axis_size("dp") == 2
    if pairs and lax.axis_size("seq") == 8 and heads % 8 == 0:
        return by_halves(*arrays)
    return by_tokens(*arrays)


def solution(mesh):
    placed = (
        P("dp", "seq", "tp"),
        P("dp", "seq", "tp"),
        P("dp", "seq", None),
        P("seq", "tp"),
        P("seq", "tp"),
        P("seq", "tp"),
        P("dp", None),
        P("dp", None),
    )
    return jax.shard_map(
        on_device,
        mesh=mesh,
        in_specs=placed,
        out_specs=(P("dp", "seq", "tp"), P("seq", "tp"), P("seq", "tp")),
        check_vma=False,
    )
```

```python
import functools
import math

import jax
import jax.numpy as jnp
import numpy as np
from jax import lax
from jax.experimental import pallas as pl
from jax.experimental.pallas import tpu as pltpu
from jax.sharding import PartitionSpec as P

NOPE = 128
ROPE = 64
VD = 128
CLIP = 8


rope_base = 50000.0
masked_value = -1e30


def turning(positions, width):
    steps = jnp.arange(width // 2, dtype=jnp.float32) * (2.0 / width)
    freqs = jnp.exp(-math.log(rope_base) * steps)
    angle = positions.astype(jnp.float32)[:, None] * freqs[None, :]
    return (jnp.cos(angle), jnp.sin(angle))


def rotate(values, cosine, sine):
    half = values.shape[-1] // 2
    first = values[..., :half]
    second = values[..., half:]
    return jnp.concatenate(
        [first * cosine - second * sine, second * cosine + first * sine], axis=-1
    )


def positions_of(index, order, half_block):
    which = index // half_block
    onehot = which[:, None] == jnp.arange(order.shape[0], dtype=jnp.int32)[None, :]
    base = jnp.sum(jnp.where(onehot, order[None, :], 0), axis=1)
    return base * half_block + index % half_block


def by_tokens(query_latent, key_latent, rope_key, w_uq, w_uk, w_uv, block_order, segment_ids):
    query_local, key_local = (
        lax.all_gather(query_latent[0], "tp", axis=1, tiled=True),
        lax.all_gather(key_latent[0], "tp", axis=1, tiled=True),
    )
    rows_uq, rows_uk, rows_uv = (
        lax.all_gather(w_uq, "seq", axis=0, tiled=True),
        lax.all_gather(w_uk, "seq", axis=0, tiled=True),
        lax.all_gather(w_uv, "seq", axis=0, tiled=True),
    )
    tok_rows = query_local.shape[0]
    half_block = tok_rows // 2
    order = block_order[0]
    labels_all = segment_ids[0]
    heads = w_uq.shape[1] // (NOPE + ROPE)
    scale = 1.0 / math.sqrt(NOPE + ROPE)
    own_index = lax.axis_index("seq") * tok_rows + jnp.arange(tok_rows, dtype=jnp.int32)
    query_pos = positions_of(own_index, order, half_block)
    query_labels = jnp.take(labels_all, query_pos)
    cosine, sine = turning(query_pos, ROPE)
    query_full = jnp.dot(query_local, rows_uq, preferred_element_type=jnp.float32).reshape(
        tok_rows, heads, NOPE + ROPE
    )
    query_nope = jnp.transpose(query_full[:, :, :NOPE].astype(jnp.bfloat16), (1, 0, 2))
    query_rope = jnp.transpose(
        rotate(query_full[:, :, NOPE:], cosine[:, None, :], sine[:, None, :]).astype(jnp.bfloat16),
        (1, 0, 2),
    )
    key_rope = rotate(rope_key[0].astype(jnp.float32), cosine, sine).astype(jnp.bfloat16)

    def slice_latent(pieces, first, width):
        latent_block = lax.dynamic_slice_in_dim(pieces[0], first, width, 0)
        rope_block = lax.dynamic_slice_in_dim(pieces[1], first, width, 0)
        nope_block = jnp.dot(latent_block, rows_uk, preferred_element_type=jnp.float32).astype(
            jnp.bfloat16
        )
        value_block = jnp.dot(latent_block, rows_uv, preferred_element_type=jnp.float32).astype(
            jnp.bfloat16
        )
        return (nope_block, value_block, rope_block)

    initial = (
        jnp.full((heads, tok_rows), masked_value, jnp.float32),
        jnp.zeros((heads, tok_rows), jnp.float32),
        jnp.zeros((heads, tok_rows, VD), jnp.float32),
    )
    pieces = (
        lax.all_gather(key_local, "seq", axis=0, tiled=True),
        lax.all_gather(key_rope, "seq", axis=0, tiled=True),
    )
    count = pieces[-1].shape[0]
    width = math.gcd(count, 512)

    def block_step(state, number):
        first = number * width
        nope_block, value_block, rope_block = slice_latent(pieces, first, width)
        nope_block = nope_block.reshape(width, heads, NOPE)
        value_block = value_block.reshape(width, heads, VD)
        key_index = first + jnp.arange(width, dtype=jnp.int32)
        key_pos = positions_of(key_index, order, half_block)
        key_labels = jnp.take(labels_all, key_pos)
        allowed = (key_pos[None, :] <= query_pos[:, None]) & (
            key_labels[None, :] == query_labels[:, None]
        )
        scores = jnp.einsum(
            "hqd,khd->hqk", query_nope, nope_block, preferred_element_type=jnp.float32
        )
        scores = (
            scores
            + jnp.einsum("hqr,kr->hqk", query_rope, rope_block, preferred_element_type=jnp.float32)
        ) * scale
        masked = jnp.where(allowed[None], scores, masked_value)
        run_max, run_total, run_sum = state
        new_max = jnp.maximum(run_max, jnp.max(masked, axis=2))
        weights = jnp.where(allowed[None], jnp.exp(masked - new_max[:, :, None]), 0.0)
        shrink = jnp.exp(run_max - new_max)
        new_total = run_total * shrink + jnp.sum(weights, axis=2)
        mixed = jnp.einsum(
            "hqk,khv->hqv",
            weights.astype(jnp.bfloat16),
            value_block,
            preferred_element_type=jnp.float32,
        )
        new_sum = run_sum * shrink[:, :, None] + mixed
        return ((new_max, new_total, new_sum), None)

    result, unused = lax.scan(block_step, initial, jnp.arange(count // width, dtype=jnp.int32))
    run_max, run_total, run_sum = result
    context = (run_sum / run_total[:, :, None]).astype(jnp.bfloat16)
    context = jnp.transpose(context, (1, 0, 2)).reshape(1, tok_rows, heads * VD)
    head_max = lax.pmax(jnp.max(run_max, axis=1), ("seq", "dp"))
    ratio = CLIP / jnp.maximum(head_max, CLIP)
    root = jnp.sqrt(ratio)
    factors = jnp.concatenate(
        [
            jnp.broadcast_to(root[:, None], (heads, NOPE)),
            jnp.broadcast_to(ratio[:, None], (heads, ROPE)),
        ],
        axis=1,
    ).reshape(heads * (NOPE + ROPE))
    clipped_uq = (w_uq.astype(jnp.float32) * factors[None, :]).astype(jnp.bfloat16)
    clipped_uk = (w_uk.astype(jnp.float32) * jnp.repeat(root, NOPE)[None, :]).astype(jnp.bfloat16)
    return (context, clipped_uq, clipped_uk)


def turned(values, cosine, sine):
    half = values.shape[-1] // 2
    swapped = jnp.concatenate([values[:, half:], values[:, :half]], axis=1)
    return values * cosine + swapped * sine


MESH = pl.DeviceIdType.MESH


def window(start, size):
    return pl.ds(pl.multiple_of(start * size, size), size)


def greet(wheres):
    barrier = pltpu.get_barrier_semaphore()
    for where in wheres:
        pl.semaphore_signal(barrier, inc=1, device_id=where, device_id_type=MESH)
    pl.semaphore_wait(barrier, len(wheres))


def fused(
    n, block, groups,
    order, label_ref, query_ref, key_ref, rope_ref, uq_ref, uk_ref, uv_ref, turn_ref,
    out_ref, peaks_ref,
    q_lat, k_lat, r_lat, r_blk, wq_s, wk_s, wv_s, wvt_s, wide_s, q_s, k_s, vt_s, s_s, p_s, c_s, lab_s, turn_s,
    peak_s, inv_s,
    got_q, got_k, got_r, got_w, got_c, got_p,
    sent_l, sent_w, sent_x, sent_m, sent_c, sent_p, local_l, local_w, local_c,
):
    s, t, d = lax.axis_index("seq"), lax.axis_index("tp"), lax.axis_index("dp")
    quarter = n // 2
    level, core = s // 2, lax.rem(s, 2)
    half = s // quarter
    place = lax.rem(s, quarter)
    first_of_half = half * quarter
    mate = s + 1 - 2 * core
    pair = first_of_half + lax.rem(place + 2, quarter)
    inner = (level == quarter // 2 - 1) | (level == quarter // 2)
    gate = jnp.where(half == 0, quarter, quarter - 2) + core
    far = [(1 - half) * quarter + 2 * k + core for k in range(2)]
    others = [lax.rem(s + k, n) for k in range(1, n)]
    to_mate, to_pair, to_gate = {"seq": mate}, {"seq": pair}, {"seq": gate}
    beside, across = {"tp": 1 - t}, {"dp": 1 - d}
    peers = [{"seq": to} for to in others] + [across] + [{"seq": to, "dp": 1 - d} for to in others]
    greet(peers + [beside])

    rows, wide = query_ref.shape
    part, unused, thin = key_ref.shape
    blocks = k_lat.shape[0]
    count = blocks * block
    own_blocks = blocks // 2
    back = blocks // 2
    scale = 1.0 / math.sqrt(NOPE + ROPE)
    turn_width = NOPE + ROPE

    def link(source, target, arrived, where, sender):
        return pltpu.make_async_remote_copy(
            src_ref=source, dst_ref=target, send_sem=sender, recv_sem=arrived,
            device_id=where, device_id_type=MESH,
        )

    def arrive(target, arrived):
        link(target, target, arrived, beside, sent_l.at[0]).wait_recv()

    started = []
    state = {"when": None}

    def send(source, spot, where):
        target, arrived = spot()
        source = target if source is None else source
        link(source, target, arrived, where, sent_l.at[len(started)]).start()
        started.append((spot, where, state["when"]))

    def under(condition, action):
        state["when"] = condition
        pl.when(condition)(action)
        state["when"] = None

    def q_spot(src, tp):
        at = lax.rem(src, quarter)
        return (q_lat.at[window(at, rows), window(tp, wide)], got_q.at[at, tp])

    def k_spot(src, tp):
        return (k_lat.at[window(src, part), :, window(tp, thin)], got_k.at[src, tp])

    def r_spot(src):
        return (r_lat.at[:, window(src, rows)], got_r.at[src])

    for where in (to_gate, to_pair):
        send(key_ref, lambda: k_spot(s, t), where)
        send(rope_ref, lambda: r_spot(s), where)
    send(query_ref, lambda: q_spot(s, t), to_pair)
    send(key_ref, lambda: k_spot(s, t), beside)
    send(query_ref, lambda: q_spot(s, t), beside)
    send(key_ref, lambda: k_spot(s, t), to_mate)
    send(rope_ref, lambda: r_spot(s), to_mate)
    send(query_ref, lambda: q_spot(s, t), to_mate)

    weights = ((uk_ref, wk_s), (uv_ref, wv_s), (uq_ref, wq_s))

    def w_spot(g, index, src):
        ref, held = weights[index]
        return (held.at[g, window(src, ref.shape[0]), :], got_w.at[g, index, src])

    def w_piece(g, index, to):
        ref, held = weights[index]
        return ref.at[:, window(lax.rem(to, quarter) * groups + g, held.shape[2])]

    def w_copy(g, index, slot, to):
        target, arrived = w_spot(g, index, s)
        return link(w_piece(g, index, to), target, arrived, {"seq": to}, sent_w.at[g, index, slot])

    far_to = [
        (1 - half) * quarter + lax.rem(k + 2 * lax.rem(level, 2), quarter) for k in range(quarter)
    ]
    pair_chip = pair - core
    near_to = [pair_chip, pair_chip + 1]
    sender = core == d

    def far_copies(g, first=0):
        return [w_copy(g, i, k, far_to[k]) for k in range(first, first + 2) for i in range(3)]

    def near_copies(g):
        return [w_copy(g, i, quarter + k, to) for k, to in enumerate(near_to) for i in range(3)]

    def start_all(copies):
        for copy in copies:
            copy.start()

    def send_weights(g):
        start_all(near_copies(g) + far_copies(g, 0))
        pl.when(~inner)(lambda: start_all(far_copies(g, 2)))
        pl.when(inner & (g + 1 < groups))(lambda: start_all(far_copies(g + 1, 2)))

    pl.when(sender & ~inner)(lambda: start_all(near_copies(0)))
    pl.when(sender)(lambda: start_all(far_copies(0, 0) + far_copies(0, 2)))
    pl.when(sender & inner)(lambda: start_all(far_copies(1, 2)))


    def mate_copies(g):
        out = []
        for i in range(3):
            target, arrived = w_spot(g, i, s)
            out.append(link(w_piece(g, i, mate), target, arrived, to_mate, sent_m.at[g, i]))
        return out

    def kept_weights(g):
        return [
            pltpu.make_async_copy(w_piece(g, i, s), w_spot(g, i, s)[0], local_w.at[g, i])
            for i in range(3)
        ]

    def near_weights(g, unused):
        start_all(kept_weights(g))
        start_all(mate_copies(g))
        return unused

    lax.fori_loop(0, groups, near_weights, 0)

    kept = [
        pltpu.make_async_copy(key_ref, k_spot(s, t)[0], local_l.at[0]),
        pltpu.make_async_copy(rope_ref, r_spot(s)[0], local_l.at[1]),
        pltpu.make_async_copy(query_ref, q_spot(s, t)[0], local_l.at[2]),
        pltpu.make_async_copy(turn_ref, turn_s, local_l.at[3]),
    ]
    start_all(kept)

    def label_step(p, unused):
        at = 0
        for b in range(blocks):
            at = jnp.where(order[b] == p, b, at)
        inv_s[p] = at
        lab_s[back + p] = jnp.transpose(jnp.broadcast_to(label_ref[p], (block, block)))
        return unused

    lax.fori_loop(0, blocks, label_step, 0)

    def empty_step(p, unused):
        lab_s[p] = jnp.full((block, block), -1, jnp.int32)
        for head in range(2):
            k_s[head, p] = jnp.zeros((block, turn_width), jnp.bfloat16)
        vt_s[p] = jnp.zeros((2 * VD, block), jnp.bfloat16)
        return unused

    lax.fori_loop(0, back, empty_step, 0)

    def pass_keys(src, onward):
        arrive(*k_spot(src, t))
        arrive(*r_spot(src))
        if onward:
            send(None, lambda: k_spot(src, t), to_pair)
            send(None, lambda: r_spot(src), to_pair)
        send(None, lambda: k_spot(src, t), beside)
        send(None, lambda: k_spot(src, t), to_mate)
        send(None, lambda: r_spot(src), to_mate)

    def hand_keys(src):
        arrive(*k_spot(src, 1 - t))
        send(None, lambda: k_spot(src, 1 - t), to_mate)

    def hand_query(src):
        arrive(*q_spot(src, 1 - t))
        send(None, lambda: q_spot(src, 1 - t), to_mate)

    def turn_ropes():
        for b in range(blocks):
            r_blk[b] = r_lat[:, b * block : (b + 1) * block]

        def rope_step(p, unused):
            raw = jnp.transpose(r_blk[inv_s[p]].astype(jnp.float32))
            turned_key = turned(raw, turn_s[p, :, :ROPE], turn_s[p, :, ROPE:]).astype(jnp.bfloat16)
            for head in range(2):
                k_s[head, p + back, :, NOPE:] = turned_key
            return unused

        lax.fori_loop(0, blocks, rope_step, 0)

    across_from = [pair_chip, gate - core, 2 * (1 - half) * quarter + quarter - 2 - (gate - core)]

    def forward(g, k):
        src = across_from[k] + d
        for i in range(3):
            target, arrived = w_spot(g, i, src)
            arrive(target, arrived)
            link(target, target, arrived, across, sent_x.at[g, i, k]).start()

    def pass_query():
        arrive(*q_spot(pair, t))
        send(None, lambda: q_spot(pair, t), beside)
        send(None, lambda: q_spot(pair, t), to_mate)

    def relay():
        for src in far:
            pass_keys(src, True)

    def take():
        for src in far:
            pass_keys(src, False)

    pass_keys(pair, False)
    under(inner, relay)
    pl.when(sender & inner)(lambda: start_all(near_copies(0)))
    hand_keys(s)
    hand_query(s)
    pass_query()
    hand_keys(pair)
    forward(0, 1)
    pl.when(sender)(lambda: send_weights(1))
    forward(0, 2)
    under(~inner, take)
    for src in far:
        hand_keys(src)
    hand_query(pair)
    forward(0, 0)
    pl.when(sender)(lambda: send_weights(2))

    for k in range(quarter):
        src = 2 * k + 1 - core
        arrive(*k_spot(src, t))
        arrive(*k_spot(src, 1 - t))
        arrive(*r_spot(src))
    for copy in kept:
        copy.wait()
    turn_ropes()
    for src in (mate, pair + 1 - 2 * core):
        arrive(*q_spot(src, t))
        arrive(*q_spot(src, 1 - t))

    step_blocks = 4
    devices_rows = uq_ref.shape[0]
    chunk = step_blocks * block
    factor = scale * math.log2(math.e)

    def out_spot(g, src):
        at = lax.rem(src, quarter)
        return (out_ref.at[:, window(at * groups + g, 2 * VD)], got_c.at[g, at])

    other_chip = lax.rem(place - core + 2, quarter)

    def context_to(g, k):
        at = lax.rem(other_chip + k, quarter)
        target, arrived = out_spot(g, s)
        return link(
            c_s.at[g, window(at, rows), :], target, arrived,
            {"seq": first_of_half + at}, sent_c.at[g, k],
        )

    def kept_context(g):
        return pltpu.make_async_copy(
            c_s.at[g, window(place, rows), :], out_spot(g, s)[0], local_c.at[g]
        )

    def leave(g, k):
        if k < 2:
            context_to(g, k).start()
        else:
            pl.when(core == k - 2)(kept_context(g).start)
            pl.when(core != k - 2)(context_to(g, k).start)

    def left(g):
        for k in range(2):
            context_to(g, k).wait_send()
        for k in range(2, 4):
            pl.when(core != k - 2)(context_to(g, k).wait_send)
        kept_context(g).wait()

    held = inner & ~sender
    onward_at = ("keys", "queries", 1)

    def group(g, unused):
        pl.when(sender & (g + 3 < groups))(lambda: send_weights(g + 3))
        def await_weights(i):
            for k in range(len(across_from)):
                arrive(*w_spot(g, i, across_from[k] + 1 - d))
            arrive(*w_spot(g, i, mate))
            kept_weights(g)[i].wait()

        for i in range(2):
            await_weights(i)

        def onward(where):
            for k in range(3):
                if onward_at[k] == where:
                    pl.when(g + 1 < groups)(lambda k=k: forward(g + 1, k))

        @pl.when(held & (g >= 2))
        def _():
            for k in range(2):
                leave(g - 2, k)

        @pl.when(held & (g + 1 == groups))
        def _():
            for k in range(2):
                leave(g - 1, k)

        onward("start")
        wvt_s[...] = jnp.transpose(wv_s[g])

        def keys(step, unused):
            latent = jnp.concatenate(
                [k_lat[inv_s[step * step_blocks + j]] for j in range(step_blocks)], axis=0
            )
            nope = jnp.dot(latent, wk_s[g], preferred_element_type=jnp.float32)
            nope = nope.astype(jnp.bfloat16)
            value = lax.dot_general(
                wvt_s[...], latent, (((1,), (1,)), ((), ())), preferred_element_type=jnp.float32
            )
            value = value.astype(jnp.bfloat16)
            for j in range(step_blocks):
                at, lo, hi = back + step * step_blocks + j, j * block, (j + 1) * block
                for head in range(2):
                    k_s[head, at, :, :NOPE] = nope[lo:hi, head * NOPE : (head + 1) * NOPE]
                vt_s[at] = value[:, lo:hi]
            return unused

        lax.fori_loop(0, blocks // step_blocks, keys, 0)
        onward("keys")

        def widen(step, unused):
            here = window(step, devices_rows)
            raw = wq_s[g, here, :]
            pieces = []
            for head in range(2):
                base = head * turn_width
                rope = base + NOPE
                middle = rope + ROPE // 2
                pieces += [
                    raw[:, base:rope], raw[:, rope : rope + ROPE],
                    raw[:, middle : rope + ROPE], raw[:, rope:middle],
                ]
            wide_s[here, :] = jnp.concatenate(pieces, axis=1)
            return unused

        await_weights(2)
        lax.fori_loop(0, n, widen, 0)

        def queries(step, unused):
            full = jnp.dot(
                q_lat[window(step, chunk), :], wide_s[...], preferred_element_type=jnp.float32
            )
            for j in range(step_blocks):
                b = step * step_blocks + j
                turns = turn_s[order[half * own_blocks + b]]
                lo, hi = j * block, (j + 1) * block
                here = window(b, block)
                for head in range(2):
                    base = head * 2 * NOPE
                    q_s[head, here, :NOPE] = full[lo:hi, base : base + NOPE].astype(jnp.bfloat16)
                    both = full[lo:hi, base + NOPE : base + 2 * NOPE] * turns
                    q_s[head, here, NOPE:] = (both[:, :ROPE] + both[:, ROPE:]).astype(
                        jnp.bfloat16
                    )
            return unused

        lax.fori_loop(0, own_blocks // step_blocks, queries, 0)
        onward("queries")

        causal = lax.broadcasted_iota(jnp.int32, (block, block), 0) <= (
            lax.broadcasted_iota(jnp.int32, (block, block), 1)
        )

        def place_of(step):
            b = lax.rem(other_chip * part + step, own_blocks)
            return window(b, block), order[half * own_blocks + b]

        def score(step, slot):
            here, p = place_of(step)
            asking = label_ref[p]
            raws = [
                lax.dot_general(
                    jnp.concatenate([k_s[head, p + j] for j in range(back + 1)], axis=0),
                    q_s[head, here, :], (((1,), (1,)), ((), ())),
                    preferred_element_type=jnp.float32,
                )
                for head in range(2)
            ]
            tops = [jnp.full((8, block), masked_value, jnp.float32) for head in range(2)]
            for j in range(back + 1):
                lo, hi = j * block, (j + 1) * block
                allowed = lab_s[p + j] == asking
                if j == back:
                    allowed = allowed & causal
                for head in range(2):
                    raw = jnp.where(allowed, raws[head][lo:hi, :], masked_value)
                    s_s[slot, head, lo:hi, :] = raw
                    tops[head] = jnp.maximum(
                        tops[head], jnp.max(raw.reshape(block // 8, 8, block), axis=0)
                    )
            return tuple(jnp.max(tops[head], axis=0, keepdims=True) for head in range(2))

        def mix(step, slot, tops, best):
            here, p = place_of(step)
            for head in range(2):
                top = tops[head]
                total = jnp.zeros((8, block), jnp.float32)
                for j in range(back + 1):
                    lo, hi = j * block, (j + 1) * block
                    piece = jnp.exp2((s_s[slot, head, lo:hi, :] - top) * factor)
                    total = total + jnp.sum(piece.reshape(block // 8, 8, block), axis=0)
                    p_s[slot, head, lo:hi, :] = piece.astype(jnp.bfloat16)
                mixed = jnp.dot(
                    jnp.concatenate(
                        [vt_s[p + j, head * VD : (head + 1) * VD, :] for j in range(back + 1)], axis=1
                    ),
                    p_s[slot, head],
                    preferred_element_type=jnp.float32,
                )
                done = mixed / jnp.sum(total, axis=0, keepdims=True)
                c_s[g, here, head * VD : (head + 1) * VD] = jnp.transpose(done).astype(
                    jnp.bfloat16
                )
            return tuple(jnp.maximum(best[head], tops[head]) for head in range(2))

        def attend(turn, carried):
            tops, best = carried
            for slot in range(2):
                step = 2 * turn + slot
                later = score(step + 1, 1 - slot)
                best = mix(step, slot, tops, best)
                tops = later
            for k in range(2):
                pl.when((turn == k + 1) & (~held | (g + 1 == groups)))(lambda k=k: leave(g, k))
            for k in range(3):
                at = onward_at[k]
                if isinstance(at, int):
                    pl.when((turn == at) & (g + 1 < groups))(lambda k=k: forward(g + 1, k))
            return (tops, best)

        low = jnp.full((1, block), masked_value, jnp.float32)
        rounds = own_blocks // 2 - 1
        tops, best = lax.fori_loop(0, rounds, attend, (score(0, 0), (low, low)))
        onward("six")
        later = score(2 * rounds + 1, 1)
        best = mix(2 * rounds, 0, tops, best)
        leave(g, 2)
        best = mix(2 * rounds + 1, 1, later, best)
        peak_s[g] = jnp.concatenate(best, axis=0) * scale
        leave(g, 3)
        onward("end")
        return unused

    lax.fori_loop(0, groups, group, 0)

    me = d * n + s
    peak_copies = [
        link(peak_s, peaks_ref.at[me], got_p.at[me], where, sent_p.at[k])
        for k, where in enumerate(peers)
    ]
    start_all(peak_copies)
    keep_peak = pltpu.make_async_copy(peak_s, peaks_ref.at[me], local_l.at[4])
    keep_peak.start()

    def settle(g, unused):
        def far_sent():
            for copy in far_copies(g, 0) + far_copies(g, 2) + near_copies(g):
                copy.wait_send()

        pl.when(sender)(far_sent)
        for copy in mate_copies(g):
            copy.wait_send()
        for k in range(len(across_from)):
            for i in range(3):
                target, arrived = w_spot(g, i, across_from[k] + d)
                link(target, target, arrived, across, sent_x.at[g, i, k]).wait_send()
        left(g)
        for k in range(1, quarter):
            arrive(*out_spot(g, first_of_half + lax.rem(place + k, quarter)))
        return unused

    lax.fori_loop(0, groups, settle, 0)
    for k, (spot, where, condition) in enumerate(started):
        target, arrived = spot()
        copy = link(target, target, arrived, where, sent_l.at[k])
        if condition is None:
            copy.wait_send()
        else:
            pl.when(condition)(copy.wait_send)
    for copy in peak_copies:
        copy.wait_send()
    keep_peak.wait()
    for src in [d * n + to for to in others] + [(1 - d) * n + to for to in others] + [(1 - d) * n + s]:
        arrive(peaks_ref.at[src], got_p.at[src])


def by_halves(query_latent, key_latent, rope_key, w_uq, w_uk, w_uv, block_order, segment_ids):
    devices = lax.axis_size("seq")
    sides = lax.axis_size("tp")
    heads = w_uq.shape[1] // (NOPE + ROPE)
    quarter = devices // 2
    groups = heads // quarter // 2
    rows = query_latent.shape[1]
    order, labels = block_order[0], segment_ids[0]
    count, blocks = labels.shape[0], order.shape[0]
    block = count // blocks
    back = blocks // 2
    anyplace = pl.BlockSpec(memory_space=pl.ANY)
    vmem = pl.BlockSpec(memory_space=pltpu.VMEM)
    smem = pl.BlockSpec(memory_space=pltpu.SMEM)
    steps = np.arange(ROPE // 2, dtype=np.float32) * np.float32(2.0 / ROPE)
    freqs = np.exp(np.float32(-math.log(rope_base)) * steps).astype(np.float32)
    angle = np.arange(count, dtype=np.float32)[:, None] * freqs[None, :]
    cosine, sine = np.cos(angle), np.sin(angle)
    turns = jnp.asarray(np.concatenate([cosine, cosine, -sine, sine], axis=1), jnp.float32)
    bf, f32 = jnp.bfloat16, jnp.float32
    beside = 2 * (rows * heads * VD + w_uq.size + w_uk.size) + 8 * devices * groups * 2 * block
    grant = 67043328 - beside - 384 * 1024
    dma = pltpu.SemaphoreType.DMA
    context, peaks = pl.pallas_call(
        functools.partial(fused, devices, block, groups),
        out_shape=[
            pltpu.VMEM((rows, heads * VD), bf),
            pltpu.VMEM((2 * devices, groups, 2, block), f32),
        ],
        in_specs=[smem, vmem] + [anyplace] * 7,
        out_specs=[vmem, vmem],
        scratch_shapes=[
            pltpu.VMEM((count // 2, sides * query_latent.shape[2]), bf),
            pltpu.VMEM((blocks, block, sides * key_latent.shape[2]), bf),
            pltpu.VMEM((ROPE, count), bf),
            pltpu.VMEM((blocks, ROPE, block), bf),
            pltpu.VMEM((groups, devices * w_uq.shape[0], 2 * (NOPE + ROPE)), bf),
            pltpu.VMEM((groups, devices * w_uk.shape[0], 2 * NOPE), bf),
            pltpu.VMEM((groups, devices * w_uv.shape[0], 2 * VD), bf),
            pltpu.VMEM((2 * VD, devices * w_uv.shape[0]), bf),
            pltpu.VMEM((devices * w_uq.shape[0], 4 * NOPE), bf),
            pltpu.VMEM((2, count // 2, NOPE + ROPE), bf),
            pltpu.VMEM((2, back + blocks, block, NOPE + ROPE), bf),
            pltpu.VMEM((back + blocks, 2 * VD, block), bf),
            pltpu.VMEM((2, 2, (back + 1) * block, block), f32),
            pltpu.VMEM((2, 2, (back + 1) * block, block), bf),
            pltpu.VMEM((groups, count // 2, 2 * VD), bf),
            pltpu.VMEM((back + blocks, block, block), jnp.int32),
            pltpu.VMEM((blocks, block, 2 * ROPE), f32),
            pltpu.VMEM((groups, 2, block), f32),
            pltpu.SMEM((blocks,), jnp.int32),
            dma((quarter, sides)),
            dma((devices, sides)),
            dma((devices,)),
            dma((groups, 3, devices)),
            dma((groups, quarter)),
            dma((2 * devices,)),
            dma((40,)),
            dma((groups, 3, quarter + 2)),
            dma((groups, 3, quarter - 1)),
            dma((groups, 3)),
            dma((groups, quarter)),
            dma((2 * devices,)),
            dma((5,)),
            dma((groups, 3)),
            dma((groups,)),
        ],
        compiler_params=pltpu.CompilerParams(
            collective_id=0, has_side_effects=True, vmem_limit_bytes=grant
        ),
        name="fused",
    )(
        order, labels.reshape(blocks, 1, block), query_latent[0],
        key_latent[0].reshape(rows // block, block, key_latent.shape[2]),
        jnp.transpose(rope_key[0]), w_uq, w_uk, w_uv, turns.reshape(blocks, block, 2 * ROPE),
    )
    parts = 4
    context, clipped_uq, clipped_uk = pl.pallas_call(
        functools.partial(finish, parts, quarter),
        out_shape=[
            jax.ShapeDtypeStruct((rows, heads * VD), bf),
            jax.ShapeDtypeStruct(w_uq.shape, bf),
            jax.ShapeDtypeStruct(w_uk.shape, bf),
        ],
        in_specs=[vmem] * 4,
        out_specs=[anyplace] * 3,
        scratch_shapes=[
            pltpu.VMEM(w_uq.shape, bf),
            pltpu.VMEM(w_uk.shape, bf),
            dma((parts,)),
            dma((quarter, 2)),
        ],
        compiler_params=pltpu.CompilerParams(vmem_limit_bytes=24 * 1024 * 1024),
        name="finish",
    )(context, peaks.reshape(2 * devices, 2 * groups, block), w_uq, w_uk)
    return (context[None], clipped_uq, clipped_uk)


def finish(
    parts, quarter, context_ref, peak_ref, uq_ref, uk_ref, out_ref, cq_ref, ck_ref,
    cq_s, ck_s, gone, done,
):
    size = context_ref.shape[0] // parts
    places = [pl.ds(k * size, size) for k in range(parts)]
    go = [
        pltpu.make_async_copy(context_ref.at[at, :], out_ref.at[at, :], gone.at[k])
        for k, at in enumerate(places)
    ]
    for copy in go:
        copy.start()
    own = peak_ref.shape[1]
    lane = lax.broadcasted_iota(jnp.int32, (1, 128), 1)
    wide, thin = own * (NOPE + ROPE), own * NOPE
    sent = []
    for j in range(quarter):
        top = peak_ref[j]
        for k in range(1, peak_ref.shape[0] // quarter):
            top = jnp.maximum(top, peak_ref[j + k * quarter])
        ratio = CLIP / jnp.maximum(jnp.max(top, axis=1, keepdims=True), CLIP)
        root = jnp.broadcast_to(jnp.sqrt(ratio), (own, 128))
        ratio = jnp.broadcast_to(ratio, (own, 128))
        for head in range(0, own, 2):
            root_0, root_1 = root[head : head + 1], root[head + 1 : head + 2]
            ratio_0, ratio_1 = ratio[head : head + 1], ratio[head + 1 : head + 2]
            factors = [
                root_0,
                jnp.where(lane < ROPE, ratio_0, root_1),
                jnp.where(lane < ROPE, root_1, ratio_1),
            ]
            base = j * wide + head * (NOPE + ROPE)
            for k in range(3):
                at = slice(base + k * 128, base + (k + 1) * 128)
                cq_s[:, at] = (uq_ref[:, at].astype(jnp.float32) * factors[k]).astype(jnp.bfloat16)
            for k, factor in enumerate((root_0, root_1)):
                at = slice(j * thin + (head + k) * NOPE, j * thin + (head + k + 1) * NOPE)
                ck_s[:, at] = (uk_ref[:, at].astype(jnp.float32) * factor).astype(jnp.bfloat16)
        for k, (source, target, width) in enumerate(((cq_s, cq_ref, wide), (ck_s, ck_ref, thin))):
            at = pl.ds(j * width, width)
            copy = pltpu.make_async_copy(source.at[:, at], target.at[:, at], done.at[j, k])
            copy.start()
            sent.append(copy)
    for copy in sent + go:
        copy.wait()


def clipped(w_uq, w_uk, head_max, heads):
    ratio = CLIP / jnp.maximum(head_max, CLIP)
    root = jnp.sqrt(ratio)
    factors = jnp.concatenate(
        [
            jnp.broadcast_to(root[:, None], (heads, NOPE)),
            jnp.broadcast_to(ratio[:, None], (heads, ROPE)),
        ],
        axis=1,
    ).reshape(heads * (NOPE + ROPE))
    clipped_uq = (w_uq.astype(jnp.float32) * factors[None, :]).astype(jnp.bfloat16)
    clipped_uk = (w_uk.astype(jnp.float32) * jnp.repeat(root, NOPE)[None, :]).astype(jnp.bfloat16)
    return (clipped_uq, clipped_uk)


def on_device(*arrays):
    heads = arrays[3].shape[1] // (NOPE + ROPE)
    pairs = lax.axis_size("tp") == 2 and lax.axis_size("dp") == 2
    if pairs and lax.axis_size("seq") == 8 and heads % 8 == 0 and heads >= 16:
        return by_halves(*arrays)
    return by_tokens(*arrays)


def solution(mesh):
    placed = (
        P("dp", "seq", "tp"),
        P("dp", "seq", "tp"),
        P("dp", "seq", None),
        P("seq", "tp"),
        P("seq", "tp"),
        P("seq", "tp"),
        P("dp", None),
        P("dp", None),
    )
    return jax.shard_map(
        on_device,
        mesh=mesh,
        in_specs=placed,
        out_specs=(P("dp", "seq", "tp"), P("seq", "tp"), P("seq", "tp")),
        check_vma=False,
    )
```

```python
import functools
import math

import jax
import jax.numpy as jnp
import numpy as np
from jax import lax
from jax.experimental import pallas as pl
from jax.experimental.pallas import tpu as pltpu
from jax.sharding import PartitionSpec as P

NOPE = 128
ROPE = 64
VD = 128
CLIP = 8


rope_base = 50000.0
masked_value = -1e30


def turning(positions, width):
    steps = jnp.arange(width // 2, dtype=jnp.float32) * (2.0 / width)
    freqs = jnp.exp(-math.log(rope_base) * steps)
    angle = positions.astype(jnp.float32)[:, None] * freqs[None, :]
    return (jnp.cos(angle), jnp.sin(angle))


def rotate(values, cosine, sine):
    half = values.shape[-1] // 2
    first = values[..., :half]
    second = values[..., half:]
    return jnp.concatenate(
        [first * cosine - second * sine, second * cosine + first * sine], axis=-1
    )


def positions_of(index, order, half_block):
    which = index // half_block
    onehot = which[:, None] == jnp.arange(order.shape[0], dtype=jnp.int32)[None, :]
    base = jnp.sum(jnp.where(onehot, order[None, :], 0), axis=1)
    return base * half_block + index % half_block


def by_tokens(query_latent, key_latent, rope_key, w_uq, w_uk, w_uv, block_order, segment_ids):
    query_local, key_local = (
        lax.all_gather(query_latent[0], "tp", axis=1, tiled=True),
        lax.all_gather(key_latent[0], "tp", axis=1, tiled=True),
    )
    rows_uq, rows_uk, rows_uv = (
        lax.all_gather(w_uq, "seq", axis=0, tiled=True),
        lax.all_gather(w_uk, "seq", axis=0, tiled=True),
        lax.all_gather(w_uv, "seq", axis=0, tiled=True),
    )
    tok_rows = query_local.shape[0]
    half_block = tok_rows // 2
    order = block_order[0]
    labels_all = segment_ids[0]
    heads = w_uq.shape[1] // (NOPE + ROPE)
    scale = 1.0 / math.sqrt(NOPE + ROPE)
    own_index = lax.axis_index("seq") * tok_rows + jnp.arange(tok_rows, dtype=jnp.int32)
    query_pos = positions_of(own_index, order, half_block)
    query_labels = jnp.take(labels_all, query_pos)
    cosine, sine = turning(query_pos, ROPE)
    query_full = jnp.dot(query_local, rows_uq, preferred_element_type=jnp.float32).reshape(
        tok_rows, heads, NOPE + ROPE
    )
    query_nope = jnp.transpose(query_full[:, :, :NOPE].astype(jnp.bfloat16), (1, 0, 2))
    query_rope = jnp.transpose(
        rotate(query_full[:, :, NOPE:], cosine[:, None, :], sine[:, None, :]).astype(jnp.bfloat16),
        (1, 0, 2),
    )
    key_rope = rotate(rope_key[0].astype(jnp.float32), cosine, sine).astype(jnp.bfloat16)

    def slice_latent(pieces, first, width):
        latent_block = lax.dynamic_slice_in_dim(pieces[0], first, width, 0)
        rope_block = lax.dynamic_slice_in_dim(pieces[1], first, width, 0)
        nope_block = jnp.dot(latent_block, rows_uk, preferred_element_type=jnp.float32).astype(
            jnp.bfloat16
        )
        value_block = jnp.dot(latent_block, rows_uv, preferred_element_type=jnp.float32).astype(
            jnp.bfloat16
        )
        return (nope_block, value_block, rope_block)

    initial = (
        jnp.full((heads, tok_rows), masked_value, jnp.float32),
        jnp.zeros((heads, tok_rows), jnp.float32),
        jnp.zeros((heads, tok_rows, VD), jnp.float32),
    )
    pieces = (
        lax.all_gather(key_local, "seq", axis=0, tiled=True),
        lax.all_gather(key_rope, "seq", axis=0, tiled=True),
    )
    count = pieces[-1].shape[0]
    width = math.gcd(count, 512)

    def block_step(state, number):
        first = number * width
        nope_block, value_block, rope_block = slice_latent(pieces, first, width)
        nope_block = nope_block.reshape(width, heads, NOPE)
        value_block = value_block.reshape(width, heads, VD)
        key_index = first + jnp.arange(width, dtype=jnp.int32)
        key_pos = positions_of(key_index, order, half_block)
        key_labels = jnp.take(labels_all, key_pos)
        allowed = (key_pos[None, :] <= query_pos[:, None]) & (
            key_labels[None, :] == query_labels[:, None]
        )
        scores = jnp.einsum(
            "hqd,khd->hqk", query_nope, nope_block, preferred_element_type=jnp.float32
        )
        scores = (
            scores
            + jnp.einsum("hqr,kr->hqk", query_rope, rope_block, preferred_element_type=jnp.float32)
        ) * scale
        masked = jnp.where(allowed[None], scores, masked_value)
        run_max, run_total, run_sum = state
        new_max = jnp.maximum(run_max, jnp.max(masked, axis=2))
        weights = jnp.where(allowed[None], jnp.exp(masked - new_max[:, :, None]), 0.0)
        shrink = jnp.exp(run_max - new_max)
        new_total = run_total * shrink + jnp.sum(weights, axis=2)
        mixed = jnp.einsum(
            "hqk,khv->hqv",
            weights.astype(jnp.bfloat16),
            value_block,
            preferred_element_type=jnp.float32,
        )
        new_sum = run_sum * shrink[:, :, None] + mixed
        return ((new_max, new_total, new_sum), None)

    result, unused = lax.scan(block_step, initial, jnp.arange(count // width, dtype=jnp.int32))
    run_max, run_total, run_sum = result
    context = (run_sum / run_total[:, :, None]).astype(jnp.bfloat16)
    context = jnp.transpose(context, (1, 0, 2)).reshape(1, tok_rows, heads * VD)
    head_max = lax.pmax(jnp.max(run_max, axis=1), ("seq", "dp"))
    ratio = CLIP / jnp.maximum(head_max, CLIP)
    root = jnp.sqrt(ratio)
    factors = jnp.concatenate(
        [
            jnp.broadcast_to(root[:, None], (heads, NOPE)),
            jnp.broadcast_to(ratio[:, None], (heads, ROPE)),
        ],
        axis=1,
    ).reshape(heads * (NOPE + ROPE))
    clipped_uq = (w_uq.astype(jnp.float32) * factors[None, :]).astype(jnp.bfloat16)
    clipped_uk = (w_uk.astype(jnp.float32) * jnp.repeat(root, NOPE)[None, :]).astype(jnp.bfloat16)
    return (context, clipped_uq, clipped_uk)


def turned(values, cosine, sine):
    half = values.shape[-1] // 2
    swapped = jnp.concatenate([values[:, half:], values[:, :half]], axis=1)
    return values * cosine + swapped * sine


MESH = pl.DeviceIdType.MESH


def window(start, size):
    return pl.ds(pl.multiple_of(start * size, size), size)


def greet(wheres):
    barrier = pltpu.get_barrier_semaphore()
    for where in wheres:
        pl.semaphore_signal(barrier, inc=1, device_id=where, device_id_type=MESH)
    pl.semaphore_wait(barrier, len(wheres))


def fused(
    n, block, groups,
    order, label_ref, query_ref, key_ref, rope_ref, uq_ref, uk_ref, uv_ref, turn_ref,
    out_ref, peaks_ref,
    q_lat, k_lat, r_lat, r_blk, wq_s, wk_s, wv_s, wvt_s, q_s, k_s, vt_s, s_s, p_s, c_s, lab_s, turn_s,
    peak_s, inv_s,
    got_q, got_k, got_r, got_w, got_c, got_p,
    sent_l, sent_w, sent_x, sent_m, sent_c, sent_p, local_l, local_w, local_c,
):
    s, t, d = lax.axis_index("seq"), lax.axis_index("tp"), lax.axis_index("dp")
    quarter = n // 2
    level, core = s // 2, lax.rem(s, 2)
    half = s // quarter
    place = lax.rem(s, quarter)
    first_of_half = half * quarter
    mate = s + 1 - 2 * core
    pair = first_of_half + lax.rem(place + 2, quarter)
    inner = (level == quarter // 2 - 1) | (level == quarter // 2)
    gate = jnp.where(half == 0, quarter, quarter - 2) + core
    far = [(1 - half) * quarter + 2 * k + core for k in range(2)]
    others = [lax.rem(s + k, n) for k in range(1, n)]
    to_mate, to_pair, to_gate = {"seq": mate}, {"seq": pair}, {"seq": gate}
    beside, across = {"tp": 1 - t}, {"dp": 1 - d}
    peers = [{"seq": to} for to in others] + [across] + [{"seq": to, "dp": 1 - d} for to in others]
    greet(peers + [beside])

    rows, wide = query_ref.shape
    part, unused, thin = key_ref.shape
    blocks = k_lat.shape[0]
    count = blocks * block
    own_blocks = blocks // 2
    back = blocks // 2
    scale = 1.0 / math.sqrt(NOPE + ROPE)
    lane = lax.broadcasted_iota(jnp.int32, (block, 2 * ROPE), 1)
    quarter_turn = lax.rem(lane, ROPE) < ROPE // 2
    low_lane = lane < ROPE

    def link(source, target, arrived, where, sender):
        return pltpu.make_async_remote_copy(
            src_ref=source, dst_ref=target, send_sem=sender, recv_sem=arrived,
            device_id=where, device_id_type=MESH,
        )

    def arrive(target, arrived):
        link(target, target, arrived, beside, sent_l.at[0]).wait_recv()

    started = []
    state = {"when": None}

    def send(source, spot, where):
        target, arrived = spot()
        source = target if source is None else source
        link(source, target, arrived, where, sent_l.at[len(started)]).start()
        started.append((spot, where, state["when"]))

    def under(condition, action):
        state["when"] = condition
        pl.when(condition)(action)
        state["when"] = None

    def q_spot(src, tp):
        at = lax.rem(src, quarter)
        return (q_lat.at[window(at, rows), window(tp, wide)], got_q.at[at, tp])

    def k_spot(src, tp):
        return (k_lat.at[window(src, part), :, window(tp, thin)], got_k.at[src, tp])

    def r_spot(src):
        return (r_lat.at[:, window(src, rows)], got_r.at[src])

    for where in (to_gate, to_pair):
        send(key_ref, lambda: k_spot(s, t), where)
        send(rope_ref, lambda: r_spot(s), where)
    send(query_ref, lambda: q_spot(s, t), to_pair)
    send(key_ref, lambda: k_spot(s, t), beside)
    send(query_ref, lambda: q_spot(s, t), beside)
    send(key_ref, lambda: k_spot(s, t), to_mate)
    send(rope_ref, lambda: r_spot(s), to_mate)
    send(query_ref, lambda: q_spot(s, t), to_mate)

    weights = ((uk_ref, wk_s), (uv_ref, wv_s), (uq_ref, wq_s))

    def w_spot(g, index, src):
        ref, held = weights[index]
        return (held.at[g, window(src, ref.shape[0]), :], got_w.at[g, index, src])

    def w_piece(g, index, to):
        ref, held = weights[index]
        return ref.at[:, window(lax.rem(to, quarter) * groups + g, held.shape[2])]

    def w_copy(g, index, slot, to):
        target, arrived = w_spot(g, index, s)
        return link(w_piece(g, index, to), target, arrived, {"seq": to}, sent_w.at[g, index, slot])

    far_to = [
        (1 - half) * quarter + lax.rem(k + 2 * lax.rem(level, 2), quarter) for k in range(quarter)
    ]
    pair_chip = pair - core
    near_to = [pair_chip, pair_chip + 1]
    sender = core == d

    def far_copies(g, first=0):
        return [w_copy(g, i, k, far_to[k]) for k in range(first, first + 2) for i in range(3)]

    def near_copies(g):
        return [w_copy(g, i, quarter + k, to) for k, to in enumerate(near_to) for i in range(3)]

    def start_all(copies):
        for copy in copies:
            copy.start()

    def send_weights(g):
        start_all(near_copies(g) + far_copies(g, 0))
        pl.when(~inner)(lambda: start_all(far_copies(g, 2)))
        pl.when(inner & (g + 1 < groups))(lambda: start_all(far_copies(g + 1, 2)))

    pl.when(sender & ~inner)(lambda: start_all(near_copies(0)))
    pl.when(sender)(lambda: start_all(far_copies(0, 0) + far_copies(0, 2)))
    pl.when(sender & inner)(lambda: start_all(far_copies(1, 2)))


    def mate_copies(g):
        out = []
        for i in range(3):
            target, arrived = w_spot(g, i, s)
            out.append(link(w_piece(g, i, mate), target, arrived, to_mate, sent_m.at[g, i]))
        return out

    def kept_weights(g):
        return [
            pltpu.make_async_copy(w_piece(g, i, s), w_spot(g, i, s)[0], local_w.at[g, i])
            for i in range(3)
        ]

    def near_weights(g, unused):
        start_all(kept_weights(g))
        start_all(mate_copies(g))
        return unused

    lax.fori_loop(0, groups, near_weights, 0)

    kept = [
        pltpu.make_async_copy(key_ref, k_spot(s, t)[0], local_l.at[0]),
        pltpu.make_async_copy(rope_ref, r_spot(s)[0], local_l.at[1]),
        pltpu.make_async_copy(query_ref, q_spot(s, t)[0], local_l.at[2]),
        pltpu.make_async_copy(turn_ref, turn_s, local_l.at[3]),
    ]
    start_all(kept)

    def label_step(p, unused):
        at = 0
        for b in range(blocks):
            at = jnp.where(order[b] == p, b, at)
        inv_s[p] = at
        lab_s[back + p] = jnp.transpose(jnp.broadcast_to(label_ref[p], (block, block)))
        return unused

    lax.fori_loop(0, blocks, label_step, 0)

    def empty_step(p, unused):
        lab_s[p] = jnp.full((block, block), -1, jnp.int32)
        for head in range(2):
            k_s[head, p] = jnp.zeros((block, NOPE + 2 * ROPE), jnp.bfloat16)
        vt_s[p] = jnp.zeros((2 * VD, block), jnp.bfloat16)
        return unused

    lax.fori_loop(0, back, empty_step, 0)

    def pass_keys(src, onward):
        arrive(*k_spot(src, t))
        arrive(*r_spot(src))
        if onward:
            send(None, lambda: k_spot(src, t), to_pair)
            send(None, lambda: r_spot(src), to_pair)
        send(None, lambda: k_spot(src, t), beside)
        send(None, lambda: k_spot(src, t), to_mate)
        send(None, lambda: r_spot(src), to_mate)

    def hand_keys(src):
        arrive(*k_spot(src, 1 - t))
        send(None, lambda: k_spot(src, 1 - t), to_mate)

    def hand_query(src):
        arrive(*q_spot(src, 1 - t))
        send(None, lambda: q_spot(src, 1 - t), to_mate)

    def turned_pair(values, turns):
        swapped = jnp.where(
            quarter_turn,
            pltpu.roll(values, 2 * ROPE - ROPE // 2, 1), pltpu.roll(values, ROPE // 2, 1),
        )
        return values * turns[:, : 2 * ROPE] + swapped * turns[:, 2 * ROPE :]

    def turn_ropes():
        for b in range(blocks):
            r_blk[b] = r_lat[:, b * block : (b + 1) * block]

        def rope_step(p, unused):
            raw = r_blk[inv_s[p]].astype(jnp.float32)
            both = turned_pair(jnp.transpose(jnp.concatenate([raw, raw], axis=0)), turn_s[p])
            for head in range(2):
                k_s[head, p + back, :, NOPE:] = both.astype(jnp.bfloat16)
            return unused

        lax.fori_loop(0, blocks, rope_step, 0)

    across_from = [pair_chip, gate - core, 2 * (1 - half) * quarter + quarter - 2 - (gate - core)]

    def forward(g, k):
        src = across_from[k] + d
        for i in range(3):
            target, arrived = w_spot(g, i, src)
            arrive(target, arrived)
            link(target, target, arrived, across, sent_x.at[g, i, k]).start()

    def pass_query():
        arrive(*q_spot(pair, t))
        send(None, lambda: q_spot(pair, t), beside)
        send(None, lambda: q_spot(pair, t), to_mate)

    def relay():
        for src in far:
            pass_keys(src, True)

    def take():
        for src in far:
            pass_keys(src, False)

    pass_keys(pair, False)
    under(inner, relay)
    pl.when(sender & inner)(lambda: start_all(near_copies(0)))
    hand_keys(s)
    hand_query(s)
    pass_query()
    hand_keys(pair)
    forward(0, 1)
    pl.when(sender)(lambda: send_weights(1))
    under(~inner, take)
    for src in far:
        hand_keys(src)
    forward(0, 2)
    hand_query(pair)
    for k in range(quarter):
        src = 2 * k + 1 - core
        arrive(*k_spot(src, t))
        arrive(*k_spot(src, 1 - t))
        arrive(*r_spot(src))
    for copy in kept:
        copy.wait()
    turn_ropes()
    forward(0, 0)
    pl.when(sender)(lambda: send_weights(2))
    for src in (mate, pair + 1 - 2 * core):
        arrive(*q_spot(src, t))
        arrive(*q_spot(src, 1 - t))

    step_blocks = 4
    chunk = step_blocks * block
    factor = scale * math.log2(math.e)

    def out_spot(g, src):
        at = lax.rem(src, quarter)
        return (out_ref.at[:, window(at * groups + g, 2 * VD)], got_c.at[g, at])

    other_chip = lax.rem(place - core + 2, quarter)

    def context_to(g, k):
        at = lax.rem(other_chip + k, quarter)
        target, arrived = out_spot(g, s)
        return link(
            c_s.at[g, window(at, rows), :], target, arrived,
            {"seq": first_of_half + at}, sent_c.at[g, k],
        )

    def kept_context(g):
        return pltpu.make_async_copy(
            c_s.at[g, window(place, rows), :], out_spot(g, s)[0], local_c.at[g]
        )

    def leave(g, k):
        if k < 2:
            context_to(g, k).start()
        else:
            pl.when(core == k - 2)(kept_context(g).start)
            pl.when(core != k - 2)(context_to(g, k).start)

    def left(g):
        for k in range(2):
            context_to(g, k).wait_send()
        for k in range(2, 4):
            pl.when(core != k - 2)(context_to(g, k).wait_send)
        kept_context(g).wait()

    held = inner & ~sender
    onward_at = ("keys", "queries", 1)

    def group(g, unused):
        pl.when(sender & (g + 3 < groups))(lambda: send_weights(g + 3))
        def await_weights(i):
            for k in range(len(across_from)):
                arrive(*w_spot(g, i, across_from[k] + 1 - d))
            arrive(*w_spot(g, i, mate))
            kept_weights(g)[i].wait()

        for i in range(2):
            await_weights(i)

        def onward(where):
            for k in range(3):
                if onward_at[k] == where:
                    pl.when(g + 1 < groups)(lambda k=k: forward(g + 1, k))

        @pl.when(held & (g >= 2))
        def _():
            for k in range(2):
                leave(g - 2, k)

        @pl.when(held & (g + 1 == groups))
        def _():
            for k in range(2):
                leave(g - 1, k)

        onward("start")
        wvt_s[...] = jnp.transpose(wv_s[g])

        def keys(step, unused):
            latent = jnp.concatenate(
                [k_lat[inv_s[step * step_blocks + j]] for j in range(step_blocks)], axis=0
            )
            nope = jnp.dot(latent, wk_s[g], preferred_element_type=jnp.float32)
            nope = (nope[:, :NOPE], pltpu.roll(nope[:, NOPE:], ROPE, 1))
            value = lax.dot_general(
                wvt_s[...], latent, (((1,), (1,)), ((), ())), preferred_element_type=jnp.float32
            )
            value = value.astype(jnp.bfloat16)
            for j in range(step_blocks):
                at, lo, hi = back + step * step_blocks + j, j * block, (j + 1) * block
                for head in range(2):
                    k_s[head, at, :, :NOPE] = nope[head][lo:hi, :].astype(jnp.bfloat16)
                vt_s[at] = value[:, lo:hi]
            return unused

        lax.fori_loop(0, blocks // step_blocks, keys, 0)
        onward("keys")

        def queries(step, unused):
            full = jnp.dot(
                q_lat[window(step, chunk), :], wq_s[g], preferred_element_type=jnp.float32
            )
            for j in range(step_blocks):
                b = step * step_blocks + j
                turns = turn_s[order[half * own_blocks + b]]
                lo, hi = j * block, (j + 1) * block
                here = window(b, block)
                first, second, third = (full[lo:hi, k * NOPE : (k + 1) * NOPE] for k in range(3))
                ropes = turned_pair(jnp.where(low_lane, second, third), turns)
                q_s[0, here, :NOPE] = first.astype(jnp.bfloat16)
                q_s[1, here, :NOPE] = jnp.where(low_lane, third, second).astype(jnp.bfloat16)
                q_s[0, here, NOPE:] = jnp.where(low_lane, ropes, 0.0).astype(jnp.bfloat16)
                q_s[1, here, NOPE:] = jnp.where(low_lane, 0.0, ropes).astype(jnp.bfloat16)
            return unused

        await_weights(2)
        lax.fori_loop(0, own_blocks // step_blocks, queries, 0)
        onward("queries")

        causal = lax.broadcasted_iota(jnp.int32, (block, block), 0) <= (
            lax.broadcasted_iota(jnp.int32, (block, block), 1)
        )

        def place_of(step):
            b = lax.rem(other_chip * part + step, own_blocks)
            return window(b, block), order[half * own_blocks + b]

        def score(step, slot):
            here, p = place_of(step)
            asking = label_ref[p]
            raws = [
                lax.dot_general(
                    jnp.concatenate([k_s[head, p + j] for j in range(back + 1)], axis=0),
                    q_s[head, here, :], (((1,), (1,)), ((), ())),
                    preferred_element_type=jnp.float32,
                )
                for head in range(2)
            ]
            tops = [jnp.full((8, block), masked_value, jnp.float32) for head in range(2)]
            for j in range(back + 1):
                lo, hi = j * block, (j + 1) * block
                allowed = lab_s[p + j] == asking
                if j == back:
                    allowed = allowed & causal
                for head in range(2):
                    raw = jnp.where(allowed, raws[head][lo:hi, :], masked_value)
                    s_s[slot, head, lo:hi, :] = raw
                    tops[head] = jnp.maximum(
                        tops[head], jnp.max(raw.reshape(block // 8, 8, block), axis=0)
                    )
            return tuple(jnp.max(tops[head], axis=0, keepdims=True) for head in range(2))

        def mix(step, slot, tops, best):
            here, p = place_of(step)
            for head in range(2):
                top = tops[head]
                total = jnp.zeros((8, block), jnp.float32)
                for j in range(back + 1):
                    lo, hi = j * block, (j + 1) * block
                    piece = jnp.exp2((s_s[slot, head, lo:hi, :] - top) * factor)
                    total = total + jnp.sum(piece.reshape(block // 8, 8, block), axis=0)
                    p_s[slot, head, lo:hi, :] = piece.astype(jnp.bfloat16)
                mixed = jnp.dot(
                    jnp.concatenate(
                        [vt_s[p + j, head * VD : (head + 1) * VD, :] for j in range(back + 1)], axis=1
                    ),
                    p_s[slot, head],
                    preferred_element_type=jnp.float32,
                )
                done = mixed / jnp.sum(total, axis=0, keepdims=True)
                c_s[g, here, head * VD : (head + 1) * VD] = jnp.transpose(done).astype(
                    jnp.bfloat16
                )
            return tuple(jnp.maximum(best[head], tops[head]) for head in range(2))

        def attend(turn, carried):
            tops, best = carried
            for slot in range(2):
                step = 2 * turn + slot
                later = score(step + 1, 1 - slot)
                best = mix(step, slot, tops, best)
                tops = later
            for k in range(2):
                pl.when((turn == k + 1) & (~held | (g + 1 == groups)))(lambda k=k: leave(g, k))
            for k in range(3):
                at = onward_at[k]
                if isinstance(at, int):
                    pl.when((turn == at) & (g + 1 < groups))(lambda k=k: forward(g + 1, k))
            return (tops, best)

        low = jnp.full((1, block), masked_value, jnp.float32)
        rounds = own_blocks // 2 - 1
        tops, best = lax.fori_loop(0, rounds, attend, (score(0, 0), (low, low)))
        onward("six")
        later = score(2 * rounds + 1, 1)
        best = mix(2 * rounds, 0, tops, best)
        leave(g, 2)
        best = mix(2 * rounds + 1, 1, later, best)
        peak_s[g] = jnp.concatenate(best, axis=0) * scale
        leave(g, 3)
        onward("end")
        return unused

    lax.fori_loop(0, groups, group, 0)

    me = d * n + s
    peak_copies = [
        link(peak_s, peaks_ref.at[me], got_p.at[me], where, sent_p.at[k])
        for k, where in enumerate(peers)
    ]
    start_all(peak_copies)
    keep_peak = pltpu.make_async_copy(peak_s, peaks_ref.at[me], local_l.at[4])
    keep_peak.start()

    def settle(g, unused):
        def far_sent():
            for copy in far_copies(g, 0) + far_copies(g, 2) + near_copies(g):
                copy.wait_send()

        pl.when(sender)(far_sent)
        for copy in mate_copies(g):
            copy.wait_send()
        for k in range(len(across_from)):
            for i in range(3):
                target, arrived = w_spot(g, i, across_from[k] + d)
                link(target, target, arrived, across, sent_x.at[g, i, k]).wait_send()
        left(g)
        for k in range(1, quarter):
            arrive(*out_spot(g, first_of_half + lax.rem(place + k, quarter)))
        return unused

    lax.fori_loop(0, groups, settle, 0)
    for k, (spot, where, condition) in enumerate(started):
        target, arrived = spot()
        copy = link(target, target, arrived, where, sent_l.at[k])
        if condition is None:
            copy.wait_send()
        else:
            pl.when(condition)(copy.wait_send)
    for copy in peak_copies:
        copy.wait_send()
    keep_peak.wait()
    for src in [d * n + to for to in others] + [(1 - d) * n + to for to in others] + [(1 - d) * n + s]:
        arrive(peaks_ref.at[src], got_p.at[src])


def by_halves(query_latent, key_latent, rope_key, w_uq, w_uk, w_uv, block_order, segment_ids):
    devices = lax.axis_size("seq")
    sides = lax.axis_size("tp")
    heads = w_uq.shape[1] // (NOPE + ROPE)
    quarter = devices // 2
    groups = heads // quarter // 2
    rows = query_latent.shape[1]
    order, labels = block_order[0], segment_ids[0]
    count, blocks = labels.shape[0], order.shape[0]
    block = count // blocks
    back = blocks // 2
    anyplace = pl.BlockSpec(memory_space=pl.ANY)
    vmem = pl.BlockSpec(memory_space=pltpu.VMEM)
    smem = pl.BlockSpec(memory_space=pltpu.SMEM)
    steps = np.arange(ROPE // 2, dtype=np.float32) * np.float32(2.0 / ROPE)
    freqs = np.exp(np.float32(-math.log(rope_base)) * steps).astype(np.float32)
    angle = np.arange(count, dtype=np.float32)[:, None] * freqs[None, :]
    cosine, sine = np.cos(angle), np.sin(angle)
    table = [cosine] * 4 + [-sine, sine] * 2
    turns = jnp.asarray(np.concatenate(table, axis=1), jnp.float32)
    bf, f32 = jnp.bfloat16, jnp.float32
    beside = 2 * (rows * heads * VD + w_uq.size + w_uk.size) + 8 * devices * groups * 2 * block
    grant = 67043328 - beside - 384 * 1024
    dma = pltpu.SemaphoreType.DMA
    context, peaks = pl.pallas_call(
        functools.partial(fused, devices, block, groups),
        out_shape=[
            pltpu.VMEM((rows, heads * VD), bf),
            pltpu.VMEM((2 * devices, groups, 2, block), f32),
        ],
        in_specs=[smem, vmem] + [anyplace] * 7,
        out_specs=[vmem, vmem],
        scratch_shapes=[
            pltpu.VMEM((count // 2, sides * query_latent.shape[2]), bf),
            pltpu.VMEM((blocks, block, sides * key_latent.shape[2]), bf),
            pltpu.VMEM((ROPE, count), bf),
            pltpu.VMEM((blocks, ROPE, block), bf),
            pltpu.VMEM((groups, devices * w_uq.shape[0], 2 * (NOPE + ROPE)), bf),
            pltpu.VMEM((groups, devices * w_uk.shape[0], 2 * NOPE), bf),
            pltpu.VMEM((groups, devices * w_uv.shape[0], 2 * VD), bf),
            pltpu.VMEM((2 * VD, devices * w_uv.shape[0]), bf),
            pltpu.VMEM((2, count // 2, NOPE + 2 * ROPE), bf),
            pltpu.VMEM((2, back + blocks, block, NOPE + 2 * ROPE), bf),
            pltpu.VMEM((back + blocks, 2 * VD, block), bf),
            pltpu.VMEM((2, 2, (back + 1) * block, block), f32),
            pltpu.VMEM((2, 2, (back + 1) * block, block), bf),
            pltpu.VMEM((groups, count // 2, 2 * VD), bf),
            pltpu.VMEM((back + blocks, block, block), jnp.int32),
            pltpu.VMEM((blocks, block, 4 * ROPE), f32),
            pltpu.VMEM((groups, 2, block), f32),
            pltpu.SMEM((blocks,), jnp.int32),
            dma((quarter, sides)),
            dma((devices, sides)),
            dma((devices,)),
            dma((groups, 3, devices)),
            dma((groups, quarter)),
            dma((2 * devices,)),
            dma((40,)),
            dma((groups, 3, quarter + 2)),
            dma((groups, 3, quarter - 1)),
            dma((groups, 3)),
            dma((groups, quarter)),
            dma((2 * devices,)),
            dma((5,)),
            dma((groups, 3)),
            dma((groups,)),
        ],
        compiler_params=pltpu.CompilerParams(
            collective_id=0, has_side_effects=True, vmem_limit_bytes=grant
        ),
        name="fused",
    )(
        order, labels.reshape(blocks, 1, block), query_latent[0],
        key_latent[0].reshape(rows // block, block, key_latent.shape[2]),
        jnp.transpose(rope_key[0]), w_uq, w_uk, w_uv, turns.reshape(blocks, block, 4 * ROPE),
    )
    parts = 4
    context, clipped_uq, clipped_uk = pl.pallas_call(
        functools.partial(finish, parts, quarter),
        out_shape=[
            jax.ShapeDtypeStruct((rows, heads * VD), bf),
            jax.ShapeDtypeStruct(w_uq.shape, bf),
            jax.ShapeDtypeStruct(w_uk.shape, bf),
        ],
        in_specs=[vmem] * 4,
        out_specs=[anyplace] * 3,
        scratch_shapes=[
            pltpu.VMEM(w_uq.shape, bf),
            pltpu.VMEM(w_uk.shape, bf),
            dma((parts,)),
            dma((quarter, 2)),
        ],
        compiler_params=pltpu.CompilerParams(vmem_limit_bytes=24 * 1024 * 1024),
        name="finish",
    )(context, peaks.reshape(2 * devices, 2 * groups, block), w_uq, w_uk)
    return (context[None], clipped_uq, clipped_uk)


def finish(
    parts, quarter, context_ref, peak_ref, uq_ref, uk_ref, out_ref, cq_ref, ck_ref,
    cq_s, ck_s, gone, done,
):
    size = context_ref.shape[0] // parts
    places = [pl.ds(k * size, size) for k in range(parts)]
    go = [
        pltpu.make_async_copy(context_ref.at[at, :], out_ref.at[at, :], gone.at[k])
        for k, at in enumerate(places)
    ]
    for copy in go:
        copy.start()
    own = peak_ref.shape[1]
    lane = lax.broadcasted_iota(jnp.int32, (1, 128), 1)
    wide, thin = own * (NOPE + ROPE), own * NOPE
    sent = []
    for j in range(quarter):
        top = peak_ref[j]
        for k in range(1, peak_ref.shape[0] // quarter):
            top = jnp.maximum(top, peak_ref[j + k * quarter])
        ratio = CLIP / jnp.maximum(jnp.max(top, axis=1, keepdims=True), CLIP)
        root = jnp.broadcast_to(jnp.sqrt(ratio), (own, 128))
        ratio = jnp.broadcast_to(ratio, (own, 128))
        for head in range(0, own, 2):
            root_0, root_1 = root[head : head + 1], root[head + 1 : head + 2]
            ratio_0, ratio_1 = ratio[head : head + 1], ratio[head + 1 : head + 2]
            factors = [
                root_0,
                jnp.where(lane < ROPE, ratio_0, root_1),
                jnp.where(lane < ROPE, root_1, ratio_1),
            ]
            base = j * wide + head * (NOPE + ROPE)
            for k in range(3):
                at = slice(base + k * 128, base + (k + 1) * 128)
                cq_s[:, at] = (uq_ref[:, at].astype(jnp.float32) * factors[k]).astype(jnp.bfloat16)
            for k, factor in enumerate((root_0, root_1)):
                at = slice(j * thin + (head + k) * NOPE, j * thin + (head + k + 1) * NOPE)
                ck_s[:, at] = (uk_ref[:, at].astype(jnp.float32) * factor).astype(jnp.bfloat16)
        for k, (source, target, width) in enumerate(((cq_s, cq_ref, wide), (ck_s, ck_ref, thin))):
            at = pl.ds(j * width, width)
            copy = pltpu.make_async_copy(source.at[:, at], target.at[:, at], done.at[j, k])
            copy.start()
            sent.append(copy)
    for copy in sent + go:
        copy.wait()


def clipped(w_uq, w_uk, head_max, heads):
    ratio = CLIP / jnp.maximum(head_max, CLIP)
    root = jnp.sqrt(ratio)
    factors = jnp.concatenate(
        [
            jnp.broadcast_to(root[:, None], (heads, NOPE)),
            jnp.broadcast_to(ratio[:, None], (heads, ROPE)),
        ],
        axis=1,
    ).reshape(heads * (NOPE + ROPE))
    clipped_uq = (w_uq.astype(jnp.float32) * factors[None, :]).astype(jnp.bfloat16)
    clipped_uk = (w_uk.astype(jnp.float32) * jnp.repeat(root, NOPE)[None, :]).astype(jnp.bfloat16)
    return (clipped_uq, clipped_uk)


def on_device(*arrays):
    heads = arrays[3].shape[1] // (NOPE + ROPE)
    pairs = lax.axis_size("tp") == 2 and lax.axis_size("dp") == 2
    if pairs and lax.axis_size("seq") == 8 and heads % 8 == 0 and heads >= 16:
        return by_halves(*arrays)
    return by_tokens(*arrays)


def solution(mesh):
    placed = (
        P("dp", "seq", "tp"),
        P("dp", "seq", "tp"),
        P("dp", "seq", None),
        P("seq", "tp"),
        P("seq", "tp"),
        P("seq", "tp"),
        P("dp", None),
        P("dp", None),
    )
    return jax.shard_map(
        on_device,
        mesh=mesh,
        in_specs=placed,
        out_specs=(P("dp", "seq", "tp"), P("seq", "tp"), P("seq", "tp")),
        check_vma=False,
    )
```

```python
import functools
import math

import jax
import jax.numpy as jnp
import numpy as np
from jax import lax
from jax.experimental import pallas as pl
from jax.experimental.pallas import tpu as pltpu
from jax.sharding import PartitionSpec as P

NOPE = 128
ROPE = 64
VD = 128
CLIP = 8


rope_base = 50000.0
masked_value = -1e30


def turning(positions, width):
    steps = jnp.arange(width // 2, dtype=jnp.float32) * (2.0 / width)
    freqs = jnp.exp(-math.log(rope_base) * steps)
    angle = positions.astype(jnp.float32)[:, None] * freqs[None, :]
    return (jnp.cos(angle), jnp.sin(angle))


def rotate(values, cosine, sine):
    half = values.shape[-1] // 2
    first = values[..., :half]
    second = values[..., half:]
    return jnp.concatenate(
        [first * cosine - second * sine, second * cosine + first * sine], axis=-1
    )


def positions_of(index, order, half_block):
    which = index // half_block
    onehot = which[:, None] == jnp.arange(order.shape[0], dtype=jnp.int32)[None, :]
    base = jnp.sum(jnp.where(onehot, order[None, :], 0), axis=1)
    return base * half_block + index % half_block


def by_tokens(query_latent, key_latent, rope_key, w_uq, w_uk, w_uv, block_order, segment_ids):
    query_local, key_local = (
        lax.all_gather(query_latent[0], "tp", axis=1, tiled=True),
        lax.all_gather(key_latent[0], "tp", axis=1, tiled=True),
    )
    rows_uq, rows_uk, rows_uv = (
        lax.all_gather(w_uq, "seq", axis=0, tiled=True),
        lax.all_gather(w_uk, "seq", axis=0, tiled=True),
        lax.all_gather(w_uv, "seq", axis=0, tiled=True),
    )
    tok_rows = query_local.shape[0]
    half_block = tok_rows // 2
    order = block_order[0]
    labels_all = segment_ids[0]
    heads = w_uq.shape[1] // (NOPE + ROPE)
    scale = 1.0 / math.sqrt(NOPE + ROPE)
    own_index = lax.axis_index("seq") * tok_rows + jnp.arange(tok_rows, dtype=jnp.int32)
    query_pos = positions_of(own_index, order, half_block)
    query_labels = jnp.take(labels_all, query_pos)
    cosine, sine = turning(query_pos, ROPE)
    query_full = jnp.dot(query_local, rows_uq, preferred_element_type=jnp.float32).reshape(
        tok_rows, heads, NOPE + ROPE
    )
    query_nope = jnp.transpose(query_full[:, :, :NOPE].astype(jnp.bfloat16), (1, 0, 2))
    query_rope = jnp.transpose(
        rotate(query_full[:, :, NOPE:], cosine[:, None, :], sine[:, None, :]).astype(jnp.bfloat16),
        (1, 0, 2),
    )
    key_rope = rotate(rope_key[0].astype(jnp.float32), cosine, sine).astype(jnp.bfloat16)

    def slice_latent(pieces, first, width):
        latent_block = lax.dynamic_slice_in_dim(pieces[0], first, width, 0)
        rope_block = lax.dynamic_slice_in_dim(pieces[1], first, width, 0)
        nope_block = jnp.dot(latent_block, rows_uk, preferred_element_type=jnp.float32).astype(
            jnp.bfloat16
        )
        value_block = jnp.dot(latent_block, rows_uv, preferred_element_type=jnp.float32).astype(
            jnp.bfloat16
        )
        return (nope_block, value_block, rope_block)

    initial = (
        jnp.full((heads, tok_rows), masked_value, jnp.float32),
        jnp.zeros((heads, tok_rows), jnp.float32),
        jnp.zeros((heads, tok_rows, VD), jnp.float32),
    )
    pieces = (
        lax.all_gather(key_local, "seq", axis=0, tiled=True),
        lax.all_gather(key_rope, "seq", axis=0, tiled=True),
    )
    count = pieces[-1].shape[0]
    width = math.gcd(count, 512)

    def block_step(state, number):
        first = number * width
        nope_block, value_block, rope_block = slice_latent(pieces, first, width)
        nope_block = nope_block.reshape(width, heads, NOPE)
        value_block = value_block.reshape(width, heads, VD)
        key_index = first + jnp.arange(width, dtype=jnp.int32)
        key_pos = positions_of(key_index, order, half_block)
        key_labels = jnp.take(labels_all, key_pos)
        allowed = (key_pos[None, :] <= query_pos[:, None]) & (
            key_labels[None, :] == query_labels[:, None]
        )
        scores = jnp.einsum(
            "hqd,khd->hqk", query_nope, nope_block, preferred_element_type=jnp.float32
        )
        scores = (
            scores
            + jnp.einsum("hqr,kr->hqk", query_rope, rope_block, preferred_element_type=jnp.float32)
        ) * scale
        masked = jnp.where(allowed[None], scores, masked_value)
        run_max, run_total, run_sum = state
        new_max = jnp.maximum(run_max, jnp.max(masked, axis=2))
        weights = jnp.where(allowed[None], jnp.exp(masked - new_max[:, :, None]), 0.0)
        shrink = jnp.exp(run_max - new_max)
        new_total = run_total * shrink + jnp.sum(weights, axis=2)
        mixed = jnp.einsum(
            "hqk,khv->hqv",
            weights.astype(jnp.bfloat16),
            value_block,
            preferred_element_type=jnp.float32,
        )
        new_sum = run_sum * shrink[:, :, None] + mixed
        return ((new_max, new_total, new_sum), None)

    result, unused = lax.scan(block_step, initial, jnp.arange(count // width, dtype=jnp.int32))
    run_max, run_total, run_sum = result
    context = (run_sum / run_total[:, :, None]).astype(jnp.bfloat16)
    context = jnp.transpose(context, (1, 0, 2)).reshape(1, tok_rows, heads * VD)
    head_max = lax.pmax(jnp.max(run_max, axis=1), ("seq", "dp"))
    ratio = CLIP / jnp.maximum(head_max, CLIP)
    root = jnp.sqrt(ratio)
    factors = jnp.concatenate(
        [
            jnp.broadcast_to(root[:, None], (heads, NOPE)),
            jnp.broadcast_to(ratio[:, None], (heads, ROPE)),
        ],
        axis=1,
    ).reshape(heads * (NOPE + ROPE))
    clipped_uq = (w_uq.astype(jnp.float32) * factors[None, :]).astype(jnp.bfloat16)
    clipped_uk = (w_uk.astype(jnp.float32) * jnp.repeat(root, NOPE)[None, :]).astype(jnp.bfloat16)
    return (context, clipped_uq, clipped_uk)


def turned(values, cosine, sine):
    half = values.shape[-1] // 2
    swapped = jnp.concatenate([values[:, half:], values[:, :half]], axis=1)
    return values * cosine + swapped * sine


MESH = pl.DeviceIdType.MESH


def window(start, size):
    return pl.ds(pl.multiple_of(start * size, size), size)


def greet(wheres):
    barrier = pltpu.get_barrier_semaphore()
    for where in wheres:
        pl.semaphore_signal(barrier, inc=1, device_id=where, device_id_type=MESH)
    pl.semaphore_wait(barrier, len(wheres))


def fused(
    n, block, groups,
    order, label_ref, query_ref, key_ref, rope_ref, uq_ref, uk_ref, uv_ref, turn_ref,
    out_ref, peaks_ref,
    q_lat, k_lat, r_lat, r_blk, wq_s, wk_s, wv_s, wvt_s, q_s, k_s, vt_s, s_s, p_s, c_s, lab_s, turn_s,
    peak_s, inv_s,
    got_q, got_k, got_r, got_w, got_c, got_p,
    sent_l, sent_w, sent_x, sent_m, sent_c, sent_p, local_l, local_w, local_c,
):
    s, t, d = lax.axis_index("seq"), lax.axis_index("tp"), lax.axis_index("dp")
    quarter = n // 2
    level, core = s // 2, lax.rem(s, 2)
    half = s // quarter
    place = lax.rem(s, quarter)
    first_of_half = half * quarter
    mate = s + 1 - 2 * core
    pair = first_of_half + lax.rem(place + 2, quarter)
    inner = (level == quarter // 2 - 1) | (level == quarter // 2)
    gate = jnp.where(half == 0, quarter, quarter - 2) + core
    far = [(1 - half) * quarter + 2 * k + core for k in range(2)]
    others = [lax.rem(s + k, n) for k in range(1, n)]
    to_mate, to_pair, to_gate = {"seq": mate}, {"seq": pair}, {"seq": gate}
    beside, across = {"tp": 1 - t}, {"dp": 1 - d}
    peers = [{"seq": to} for to in others] + [across] + [{"seq": to, "dp": 1 - d} for to in others]
    greet(peers + [beside])

    rows, wide = query_ref.shape
    part, unused, thin = key_ref.shape
    blocks = k_lat.shape[0]
    count = blocks * block
    own_blocks = blocks // 2
    back = blocks // 2
    scale = 1.0 / math.sqrt(NOPE + ROPE)
    lane = lax.broadcasted_iota(jnp.int32, (block, 2 * ROPE), 1)
    quarter_turn = lax.rem(lane, ROPE) < ROPE // 2
    low_lane = lane < ROPE

    def link(source, target, arrived, where, sender):
        return pltpu.make_async_remote_copy(
            src_ref=source, dst_ref=target, send_sem=sender, recv_sem=arrived,
            device_id=where, device_id_type=MESH,
        )

    def arrive(target, arrived):
        link(target, target, arrived, beside, sent_l.at[0]).wait_recv()

    started = []
    state = {"when": None}

    def send(source, spot, where):
        target, arrived = spot()
        source = target if source is None else source
        link(source, target, arrived, where, sent_l.at[len(started)]).start()
        started.append((spot, where, state["when"]))

    def under(condition, action):
        state["when"] = condition
        pl.when(condition)(action)
        state["when"] = None

    def q_spot(src, tp):
        at = lax.rem(src, quarter)
        return (q_lat.at[window(at, rows), window(tp, wide)], got_q.at[at, tp])

    def k_spot(src, tp):
        return (k_lat.at[window(src, part), :, window(tp, thin)], got_k.at[src, tp])

    def r_spot(src):
        return (r_lat.at[:, window(src, rows)], got_r.at[src])

    for where in (to_gate, to_pair):
        send(key_ref, lambda: k_spot(s, t), where)
        send(rope_ref, lambda: r_spot(s), where)
    send(query_ref, lambda: q_spot(s, t), to_pair)
    send(key_ref, lambda: k_spot(s, t), beside)
    send(query_ref, lambda: q_spot(s, t), beside)
    send(key_ref, lambda: k_spot(s, t), to_mate)
    send(rope_ref, lambda: r_spot(s), to_mate)
    send(query_ref, lambda: q_spot(s, t), to_mate)

    weights = ((uk_ref, wk_s), (uv_ref, wv_s), (uq_ref, wq_s))

    def w_spot(g, index, src):
        ref, held = weights[index]
        return (held.at[g, window(src, ref.shape[0]), :], got_w.at[g, index, src])

    def w_piece(g, index, to):
        ref, held = weights[index]
        return ref.at[:, window(lax.rem(to, quarter) * groups + g, held.shape[2])]

    def w_copy(g, index, slot, to):
        target, arrived = w_spot(g, index, s)
        return link(w_piece(g, index, to), target, arrived, {"seq": to}, sent_w.at[g, index, slot])

    far_to = [
        (1 - half) * quarter + lax.rem(k + 2 * lax.rem(level, 2), quarter) for k in range(quarter)
    ]
    pair_chip = pair - core
    near_to = [pair_chip, pair_chip + 1]
    sender = core == d

    def far_copies(g, first=0):
        return [w_copy(g, i, k, far_to[k]) for k in range(first, first + 2) for i in range(3)]

    def near_copies(g):
        return [w_copy(g, i, quarter + k, to) for k, to in enumerate(near_to) for i in range(3)]

    def start_all(copies):
        for copy in copies:
            copy.start()

    def send_weights(g):
        start_all(near_copies(g) + far_copies(g, 0))
        pl.when(~inner)(lambda: start_all(far_copies(g, 2)))
        pl.when(inner & (g + 1 < groups))(lambda: start_all(far_copies(g + 1, 2)))

    pl.when(sender & ~inner)(lambda: start_all(near_copies(0)))
    pl.when(sender)(lambda: start_all(far_copies(0, 0) + far_copies(0, 2)))
    pl.when(sender & inner)(lambda: start_all(far_copies(1, 2)))


    def mate_copies(g):
        out = []
        for i in range(3):
            target, arrived = w_spot(g, i, s)
            out.append(link(w_piece(g, i, mate), target, arrived, to_mate, sent_m.at[g, i]))
        return out

    def kept_weights(g):
        return [
            pltpu.make_async_copy(w_piece(g, i, s), w_spot(g, i, s)[0], local_w.at[g, i])
            for i in range(3)
        ]

    def near_weights(g, unused):
        start_all(kept_weights(g))
        start_all(mate_copies(g))
        return unused

    lax.fori_loop(0, groups, near_weights, 0)

    kept = [
        pltpu.make_async_copy(key_ref, k_spot(s, t)[0], local_l.at[0]),
        pltpu.make_async_copy(rope_ref, r_spot(s)[0], local_l.at[1]),
        pltpu.make_async_copy(query_ref, q_spot(s, t)[0], local_l.at[2]),
        pltpu.make_async_copy(turn_ref, turn_s, local_l.at[3]),
    ]
    start_all(kept)

    def label_step(p, unused):
        at = 0
        for b in range(blocks):
            at = jnp.where(order[b] == p, b, at)
        inv_s[p] = at
        lab_s[back + p] = jnp.transpose(jnp.broadcast_to(label_ref[p], (block, block)))
        return unused

    lax.fori_loop(0, blocks, label_step, 0)

    def empty_step(p, unused):
        lab_s[p] = jnp.full((block, block), -1, jnp.int32)
        for head in range(2):
            k_s[head, p] = jnp.zeros((block, NOPE + 2 * ROPE), jnp.bfloat16)
        vt_s[p] = jnp.zeros((2 * VD, block), jnp.bfloat16)
        return unused

    lax.fori_loop(0, back, empty_step, 0)

    def pass_keys(src, onward):
        arrive(*k_spot(src, t))
        arrive(*r_spot(src))
        if onward:
            send(None, lambda: k_spot(src, t), to_pair)
            send(None, lambda: r_spot(src), to_pair)
        send(None, lambda: k_spot(src, t), beside)
        send(None, lambda: k_spot(src, t), to_mate)
        send(None, lambda: r_spot(src), to_mate)

    def hand_keys(src):
        arrive(*k_spot(src, 1 - t))
        send(None, lambda: k_spot(src, 1 - t), to_mate)

    def hand_query(src):
        arrive(*q_spot(src, 1 - t))
        send(None, lambda: q_spot(src, 1 - t), to_mate)

    def turned_pair(values, turns):
        swapped = jnp.where(
            quarter_turn,
            pltpu.roll(values, 2 * ROPE - ROPE // 2, 1), pltpu.roll(values, ROPE // 2, 1),
        )
        return values * turns[:, : 2 * ROPE] + swapped * turns[:, 2 * ROPE :]

    def turn_ropes():
        for b in range(blocks):
            r_blk[b] = r_lat[:, b * block : (b + 1) * block]

        def rope_step(p, unused):
            raw = r_blk[inv_s[p]].astype(jnp.float32)
            both = turned_pair(jnp.transpose(jnp.concatenate([raw, raw], axis=0)), turn_s[p])
            for head in range(2):
                k_s[head, p + back, :, NOPE:] = both.astype(jnp.bfloat16)
            return unused

        lax.fori_loop(0, blocks, rope_step, 0)

    across_from = [pair_chip, gate - core, 2 * (1 - half) * quarter + quarter - 2 - (gate - core)]

    def forward(g, k):
        src = across_from[k] + d
        for i in range(3):
            target, arrived = w_spot(g, i, src)
            arrive(target, arrived)
            link(target, target, arrived, across, sent_x.at[g, i, k]).start()

    def pass_query():
        arrive(*q_spot(pair, t))
        send(None, lambda: q_spot(pair, t), beside)
        send(None, lambda: q_spot(pair, t), to_mate)

    def relay():
        for src in far:
            pass_keys(src, True)

    def take():
        for src in far:
            pass_keys(src, False)

    pass_keys(pair, False)
    under(inner, relay)
    pl.when(sender & inner)(lambda: start_all(near_copies(0)))
    hand_keys(s)
    hand_query(s)
    pass_query()
    hand_keys(pair)
    forward(0, 1)
    pl.when(sender)(lambda: send_weights(1))
    under(~inner, take)
    for src in far:
        hand_keys(src)
    forward(0, 2)
    hand_query(pair)
    for k in range(quarter):
        src = 2 * k + 1 - core
        arrive(*k_spot(src, t))
        arrive(*k_spot(src, 1 - t))
        arrive(*r_spot(src))
    for copy in kept:
        copy.wait()
    turn_ropes()
    forward(0, 0)
    for src in (mate, pair + 1 - 2 * core):
        arrive(*q_spot(src, t))
        arrive(*q_spot(src, 1 - t))

    step_blocks = 4
    chunk = step_blocks * block
    factor = scale * math.log2(math.e)

    def out_spot(g, src):
        at = lax.rem(src, quarter)
        return (out_ref.at[:, window(at * groups + g, 2 * VD)], got_c.at[g, at])

    other_chip = lax.rem(place - core + 2, quarter)

    def context_to(g, k):
        at = lax.rem(other_chip + k, quarter)
        target, arrived = out_spot(g, s)
        return link(
            c_s.at[g, window(at, rows), :], target, arrived,
            {"seq": first_of_half + at}, sent_c.at[g, k],
        )

    def kept_context(g):
        return pltpu.make_async_copy(
            c_s.at[g, window(place, rows), :], out_spot(g, s)[0], local_c.at[g]
        )

    def leave(g, k):
        if k < 2:
            context_to(g, k).start()
        else:
            pl.when(core == k - 2)(kept_context(g).start)
            pl.when(core != k - 2)(context_to(g, k).start)

    def left(g):
        for k in range(2):
            context_to(g, k).wait_send()
        for k in range(2, 4):
            pl.when(core != k - 2)(context_to(g, k).wait_send)
        kept_context(g).wait()

    held = inner & ~sender
    onward_at = ("keys", "queries", 1)

    def group(g, unused):
        pl.when(sender & (g + 2 < groups))(lambda: send_weights(g + 2))
        def await_weights(i):
            for k in range(len(across_from)):
                arrive(*w_spot(g, i, across_from[k] + 1 - d))
            arrive(*w_spot(g, i, mate))
            kept_weights(g)[i].wait()

        for i in range(2):
            await_weights(i)

        def onward(where):
            for k in range(3):
                if onward_at[k] == where:
                    pl.when(g + 1 < groups)(lambda k=k: forward(g + 1, k))

        @pl.when(held & (g >= 2))
        def _():
            for k in range(2):
                leave(g - 2, k)

        @pl.when(held & (g + 1 == groups))
        def _():
            for k in range(2):
                leave(g - 1, k)

        onward("start")
        wvt_s[...] = jnp.transpose(wv_s[g])

        def keys(step, unused):
            latent = jnp.concatenate(
                [k_lat[inv_s[step * step_blocks + j]] for j in range(step_blocks)], axis=0
            )
            nope = jnp.dot(latent, wk_s[g], preferred_element_type=jnp.float32)
            nope = (nope[:, :NOPE], pltpu.roll(nope[:, NOPE:], ROPE, 1))
            value = lax.dot_general(
                wvt_s[...], latent, (((1,), (1,)), ((), ())), preferred_element_type=jnp.float32
            )
            value = value.astype(jnp.bfloat16)
            for j in range(step_blocks):
                at, lo, hi = back + step * step_blocks + j, j * block, (j + 1) * block
                for head in range(2):
                    k_s[head, at, :, :NOPE] = nope[head][lo:hi, :].astype(jnp.bfloat16)
                vt_s[at] = value[:, lo:hi]
            return unused

        lax.fori_loop(0, blocks // step_blocks, keys, 0)
        onward("keys")

        def queries(step, unused):
            full = jnp.dot(
                q_lat[window(step, chunk), :], wq_s[g], preferred_element_type=jnp.float32
            )
            for j in range(step_blocks):
                b = step * step_blocks + j
                turns = turn_s[order[half * own_blocks + b]]
                lo, hi = j * block, (j + 1) * block
                here = window(b, block)
                first, second, third = (full[lo:hi, k * NOPE : (k + 1) * NOPE] for k in range(3))
                ropes = turned_pair(jnp.where(low_lane, second, third), turns)
                q_s[0, here, :NOPE] = first.astype(jnp.bfloat16)
                q_s[1, here, :NOPE] = jnp.where(low_lane, third, second).astype(jnp.bfloat16)
                q_s[0, here, NOPE:] = jnp.where(low_lane, ropes, 0.0).astype(jnp.bfloat16)
                q_s[1, here, NOPE:] = jnp.where(low_lane, 0.0, ropes).astype(jnp.bfloat16)
            return unused

        await_weights(2)
        lax.fori_loop(0, own_blocks // step_blocks, queries, 0)
        onward("queries")

        causal = lax.broadcasted_iota(jnp.int32, (block, block), 0) <= (
            lax.broadcasted_iota(jnp.int32, (block, block), 1)
        )

        def place_of(step):
            b = lax.rem(other_chip * part + step, own_blocks)
            return window(b, block), order[half * own_blocks + b]

        def score(step, slot):
            here, p = place_of(step)
            asking = label_ref[p]
            raws = [
                lax.dot_general(
                    jnp.concatenate([k_s[head, p + j] for j in range(back + 1)], axis=0),
                    q_s[head, here, :], (((1,), (1,)), ((), ())),
                    preferred_element_type=jnp.float32,
                )
                for head in range(2)
            ]
            tops = [jnp.full((8, block), masked_value, jnp.float32) for head in range(2)]
            for j in range(back + 1):
                lo, hi = j * block, (j + 1) * block
                allowed = lab_s[p + j] == asking
                if j == back:
                    allowed = allowed & causal
                for head in range(2):
                    raw = jnp.where(allowed, raws[head][lo:hi, :], masked_value)
                    s_s[slot, head, lo:hi, :] = raw
                    tops[head] = jnp.maximum(
                        tops[head], jnp.max(raw.reshape(block // 8, 8, block), axis=0)
                    )
            return tuple(jnp.max(tops[head], axis=0, keepdims=True) for head in range(2))

        def mix(step, slot, tops, best):
            here, p = place_of(step)
            for head in range(2):
                top = tops[head]
                total = jnp.zeros((8, block), jnp.float32)
                for j in range(back + 1):
                    lo, hi = j * block, (j + 1) * block
                    piece = jnp.exp2((s_s[slot, head, lo:hi, :] - top) * factor)
                    total = total + jnp.sum(piece.reshape(block // 8, 8, block), axis=0)
                    p_s[slot, head, lo:hi, :] = piece.astype(jnp.bfloat16)
                mixed = jnp.dot(
                    jnp.concatenate(
                        [vt_s[p + j, head * VD : (head + 1) * VD, :] for j in range(back + 1)], axis=1
                    ),
                    p_s[slot, head],
                    preferred_element_type=jnp.float32,
                )
                done = mixed / jnp.sum(total, axis=0, keepdims=True)
                c_s[g, here, head * VD : (head + 1) * VD] = jnp.transpose(done).astype(
                    jnp.bfloat16
                )
            return tuple(jnp.maximum(best[head], tops[head]) for head in range(2))

        def attend(turn, carried):
            tops, best = carried
            for slot in range(2):
                step = 2 * turn + slot
                later = score(step + 1, 1 - slot)
                best = mix(step, slot, tops, best)
                tops = later
            for k in range(2):
                pl.when((turn == k + 1) & (~held | (g + 1 == groups)))(lambda k=k: leave(g, k))
            for k in range(3):
                at = onward_at[k]
                if isinstance(at, int):
                    pl.when((turn == at) & (g + 1 < groups))(lambda k=k: forward(g + 1, k))
            return (tops, best)

        low = jnp.full((1, block), masked_value, jnp.float32)
        rounds = own_blocks // 2 - 1
        tops, best = lax.fori_loop(0, rounds, attend, (score(0, 0), (low, low)))
        onward("six")
        later = score(2 * rounds + 1, 1)
        best = mix(2 * rounds, 0, tops, best)
        leave(g, 2)
        best = mix(2 * rounds + 1, 1, later, best)
        peak_s[g] = jnp.concatenate(best, axis=0) * scale
        leave(g, 3)
        onward("end")
        return unused

    lax.fori_loop(0, groups, group, 0)

    me = d * n + s
    peak_copies = [
        link(peak_s, peaks_ref.at[me], got_p.at[me], where, sent_p.at[k])
        for k, where in enumerate(peers)
    ]
    start_all(peak_copies)
    keep_peak = pltpu.make_async_copy(peak_s, peaks_ref.at[me], local_l.at[4])
    keep_peak.start()

    def settle(g, unused):
        def far_sent():
            for copy in far_copies(g, 0) + far_copies(g, 2) + near_copies(g):
                copy.wait_send()

        pl.when(sender)(far_sent)
        for copy in mate_copies(g):
            copy.wait_send()
        for k in range(len(across_from)):
            for i in range(3):
                target, arrived = w_spot(g, i, across_from[k] + d)
                link(target, target, arrived, across, sent_x.at[g, i, k]).wait_send()
        left(g)
        for k in range(1, quarter):
            arrive(*out_spot(g, first_of_half + lax.rem(place + k, quarter)))
        return unused

    lax.fori_loop(0, groups, settle, 0)
    for k, (spot, where, condition) in enumerate(started):
        target, arrived = spot()
        copy = link(target, target, arrived, where, sent_l.at[k])
        if condition is None:
            copy.wait_send()
        else:
            pl.when(condition)(copy.wait_send)
    for copy in peak_copies:
        copy.wait_send()
    keep_peak.wait()
    for src in [d * n + to for to in others] + [(1 - d) * n + to for to in others] + [(1 - d) * n + s]:
        arrive(peaks_ref.at[src], got_p.at[src])


def by_halves(query_latent, key_latent, rope_key, w_uq, w_uk, w_uv, block_order, segment_ids):
    devices = lax.axis_size("seq")
    sides = lax.axis_size("tp")
    heads = w_uq.shape[1] // (NOPE + ROPE)
    quarter = devices // 2
    groups = heads // quarter // 2
    rows = query_latent.shape[1]
    order, labels = block_order[0], segment_ids[0]
    count, blocks = labels.shape[0], order.shape[0]
    block = count // blocks
    back = blocks // 2
    anyplace = pl.BlockSpec(memory_space=pl.ANY)
    vmem = pl.BlockSpec(memory_space=pltpu.VMEM)
    smem = pl.BlockSpec(memory_space=pltpu.SMEM)
    steps = np.arange(ROPE // 2, dtype=np.float32) * np.float32(2.0 / ROPE)
    freqs = np.exp(np.float32(-math.log(rope_base)) * steps).astype(np.float32)
    angle = np.arange(count, dtype=np.float32)[:, None] * freqs[None, :]
    cosine, sine = np.cos(angle), np.sin(angle)
    table = [cosine] * 4 + [-sine, sine] * 2
    turns = jnp.asarray(np.concatenate(table, axis=1), jnp.float32)
    bf, f32 = jnp.bfloat16, jnp.float32
    beside = 2 * (rows * heads * VD + w_uq.size + w_uk.size) + 8 * devices * groups * 2 * block
    grant = 67043328 - beside - 384 * 1024
    dma = pltpu.SemaphoreType.DMA
    context, peaks = pl.pallas_call(
        functools.partial(fused, devices, block, groups),
        out_shape=[
            pltpu.VMEM((rows, heads * VD), bf),
            pltpu.VMEM((2 * devices, groups, 2, block), f32),
        ],
        in_specs=[smem, vmem] + [anyplace] * 7,
        out_specs=[vmem, vmem],
        scratch_shapes=[
            pltpu.VMEM((count // 2, sides * query_latent.shape[2]), bf),
            pltpu.VMEM((blocks, block, sides * key_latent.shape[2]), bf),
            pltpu.VMEM((ROPE, count), bf),
            pltpu.VMEM((blocks, ROPE, block), bf),
            pltpu.VMEM((groups, devices * w_uq.shape[0], 2 * (NOPE + ROPE)), bf),
            pltpu.VMEM((groups, devices * w_uk.shape[0], 2 * NOPE), bf),
            pltpu.VMEM((groups, devices * w_uv.shape[0], 2 * VD), bf),
            pltpu.VMEM((2 * VD, devices * w_uv.shape[0]), bf),
            pltpu.VMEM((2, count // 2, NOPE + 2 * ROPE), bf),
            pltpu.VMEM((2, back + blocks, block, NOPE + 2 * ROPE), bf),
            pltpu.VMEM((back + blocks, 2 * VD, block), bf),
            pltpu.VMEM((2, 2, (back + 1) * block, block), f32),
            pltpu.VMEM((2, 2, (back + 1) * block, block), bf),
            pltpu.VMEM((groups, count // 2, 2 * VD), bf),
            pltpu.VMEM((back + blocks, block, block), jnp.int32),
            pltpu.VMEM((blocks, block, 4 * ROPE), f32),
            pltpu.VMEM((groups, 2, block), f32),
            pltpu.SMEM((blocks,), jnp.int32),
            dma((quarter, sides)),
            dma((devices, sides)),
            dma((devices,)),
            dma((groups, 3, devices)),
            dma((groups, quarter)),
            dma((2 * devices,)),
            dma((40,)),
            dma((groups, 3, quarter + 2)),
            dma((groups, 3, quarter - 1)),
            dma((groups, 3)),
            dma((groups, quarter)),
            dma((2 * devices,)),
            dma((5,)),
            dma((groups, 3)),
            dma((groups,)),
        ],
        compiler_params=pltpu.CompilerParams(
            collective_id=0, has_side_effects=True, vmem_limit_bytes=grant
        ),
        name="fused",
    )(
        order, labels.reshape(blocks, 1, block), query_latent[0],
        key_latent[0].reshape(rows // block, block, key_latent.shape[2]),
        jnp.transpose(rope_key[0]), w_uq, w_uk, w_uv, turns.reshape(blocks, block, 4 * ROPE),
    )
    parts = 4
    context, clipped_uq, clipped_uk = pl.pallas_call(
        functools.partial(finish, parts, quarter),
        out_shape=[
            jax.ShapeDtypeStruct((rows, heads * VD), bf),
            jax.ShapeDtypeStruct(w_uq.shape, bf),
            jax.ShapeDtypeStruct(w_uk.shape, bf),
        ],
        in_specs=[vmem] * 4,
        out_specs=[anyplace] * 3,
        scratch_shapes=[
            pltpu.VMEM(w_uq.shape, bf),
            pltpu.VMEM(w_uk.shape, bf),
            dma((parts,)),
            dma((quarter, 2)),
        ],
        compiler_params=pltpu.CompilerParams(vmem_limit_bytes=24 * 1024 * 1024),
        name="finish",
    )(context, peaks.reshape(2 * devices, 2 * groups, block), w_uq, w_uk)
    return (context[None], clipped_uq, clipped_uk)


def finish(
    parts, quarter, context_ref, peak_ref, uq_ref, uk_ref, out_ref, cq_ref, ck_ref,
    cq_s, ck_s, gone, done,
):
    size = context_ref.shape[0] // parts
    places = [pl.ds(k * size, size) for k in range(parts)]
    go = [
        pltpu.make_async_copy(context_ref.at[at, :], out_ref.at[at, :], gone.at[k])
        for k, at in enumerate(places)
    ]
    for copy in go:
        copy.start()
    own = peak_ref.shape[1]
    lane = lax.broadcasted_iota(jnp.int32, (1, 128), 1)
    wide, thin = own * (NOPE + ROPE), own * NOPE
    sent = []
    for j in range(quarter):
        top = peak_ref[j]
        for k in range(1, peak_ref.shape[0] // quarter):
            top = jnp.maximum(top, peak_ref[j + k * quarter])
        ratio = CLIP / jnp.maximum(jnp.max(top, axis=1, keepdims=True), CLIP)
        root = jnp.broadcast_to(jnp.sqrt(ratio), (own, 128))
        ratio = jnp.broadcast_to(ratio, (own, 128))
        for head in range(0, own, 2):
            root_0, root_1 = root[head : head + 1], root[head + 1 : head + 2]
            ratio_0, ratio_1 = ratio[head : head + 1], ratio[head + 1 : head + 2]
            factors = [
                root_0,
                jnp.where(lane < ROPE, ratio_0, root_1),
                jnp.where(lane < ROPE, root_1, ratio_1),
            ]
            base = j * wide + head * (NOPE + ROPE)
            for k in range(3):
                at = slice(base + k * 128, base + (k + 1) * 128)
                cq_s[:, at] = (uq_ref[:, at].astype(jnp.float32) * factors[k]).astype(jnp.bfloat16)
            for k, factor in enumerate((root_0, root_1)):
                at = slice(j * thin + (head + k) * NOPE, j * thin + (head + k + 1) * NOPE)
                ck_s[:, at] = (uk_ref[:, at].astype(jnp.float32) * factor).astype(jnp.bfloat16)
        for k, (source, target, width) in enumerate(((cq_s, cq_ref, wide), (ck_s, ck_ref, thin))):
            at = pl.ds(j * width, width)
            copy = pltpu.make_async_copy(source.at[:, at], target.at[:, at], done.at[j, k])
            copy.start()
            sent.append(copy)
    for copy in sent + go:
        copy.wait()


def clipped(w_uq, w_uk, head_max, heads):
    ratio = CLIP / jnp.maximum(head_max, CLIP)
    root = jnp.sqrt(ratio)
    factors = jnp.concatenate(
        [
            jnp.broadcast_to(root[:, None], (heads, NOPE)),
            jnp.broadcast_to(ratio[:, None], (heads, ROPE)),
        ],
        axis=1,
    ).reshape(heads * (NOPE + ROPE))
    clipped_uq = (w_uq.astype(jnp.float32) * factors[None, :]).astype(jnp.bfloat16)
    clipped_uk = (w_uk.astype(jnp.float32) * jnp.repeat(root, NOPE)[None, :]).astype(jnp.bfloat16)
    return (clipped_uq, clipped_uk)


def on_device(*arrays):
    heads = arrays[3].shape[1] // (NOPE + ROPE)
    pairs = lax.axis_size("tp") == 2 and lax.axis_size("dp") == 2
    if pairs and lax.axis_size("seq") == 8 and heads % 8 == 0 and heads >= 16:
        return by_halves(*arrays)
    return by_tokens(*arrays)


def solution(mesh):
    placed = (
        P("dp", "seq", "tp"),
        P("dp", "seq", "tp"),
        P("dp", "seq", None),
        P("seq", "tp"),
        P("seq", "tp"),
        P("seq", "tp"),
        P("dp", None),
        P("dp", None),
    )
    return jax.shard_map(
        on_device,
        mesh=mesh,
        in_specs=placed,
        out_specs=(P("dp", "seq", "tp"), P("seq", "tp"), P("seq", "tp")),
        check_vma=False,
    )
```
